32 devices in a mesh: dp: 8 (over z, y), mp: 4 (over x, core).
Axes of the slice: x: 2, y: 2, z: 4, core: 2. Of those that a mesh axis runs over, the one named last changes fastest.
Arguments:
- tokens: bfloat16 [12288, 768], P('dp'), may hold values from -6 to 6
- segment_ids: int32 [12288], P('dp'), may hold values from 0 to 47, as said below
- first_gain: bfloat16 [768], replicated, may hold values from 0.25 to 1.75
- first_shift: bfloat16 [768], replicated, may hold values from -3 to 3
- qkv_weight: bfloat16 [768, 3, 768], P(None, None, 'mp'), may hold values from -0.21875 to 0.21875
- qv_bias: bfloat16 [2, 12, 64], P(None, 'mp'), may hold values from -3 to 3
- proj_weight: bfloat16 [768, 768], P('mp'), may hold values from -1.25 to 1.25
- proj_bias: bfloat16 [768], replicated, may hold values from -3 to 3
- second_gain: bfloat16 [768], replicated, may hold values from 0.25 to 1.75
- second_shift: bfloat16 [768], replicated, may hold values from -3 to 3
- up_weight: bfloat16 [768, 3072], P(None, 'mp'), may hold values from -0.21875 to 0.21875
- up_bias: bfloat16 [48, 64], P('mp'), may hold values from -3 to 3
- down_weight: bfloat16 [3072, 768], P('mp'), may hold values from -0.109375 to 0.109375
- down_bias: bfloat16 [768], replicated, may hold values from -3 to 3
- cotangent: bfloat16 [12288, 768], P('dp'), may hold values from -6 to 6
Outputs:
- layer_output: bfloat16 [12288, 768], P('dp')
- input_grad: bfloat16 [12288, 768], P('dp')
- first_gain_grad: float32 [768], P('dp')
- first_shift_grad: float32 [768], P('dp')
- qkv_weight_grad: float32 [768, 3, 768], P('dp', None, 'mp')
- qv_bias_grad: float32 [2, 12, 64], P(None, 'mp', 'dp')
- proj_weight_grad: float32 [768, 768], P('mp', 'dp')
- proj_bias_grad: float32 [768], P('dp')
- second_gain_grad: float32 [768], P('dp')
- second_shift_grad: float32 [768], P('dp')
- up_weight_grad: float32 [768, 3072], P('dp', 'mp')
- up_bias_grad: float32 [48, 64], P('mp', 'dp')
- down_weight_grad: float32 [3072, 768], P('mp', 'dp')
- down_bias_grad: float32 [768], P('dp')
The draws below stay inside these ranges and needn't reach their ends.
Inputs may be any that keep to these rules, and one draw needn't show every extreme that they name: `segment_ids`: in each sequence of 512 tokens the first 16 * r tokens carry one even id and the others that id plus one, with r from 8 to 24; different sequences have different ids.
All inputs are finite; a program needn't handle non-finite values.
Results may differ from the reference program's by a relative error of at most 0.013.
Values sent between devices are 32-bit elements; how exact they have to be, the bound alone decides.
A program may use at most 128 MiB of HBM per device.

```python
import math
import jax
import jax.numpy as jnp
from jax import lax

HEADS = 12
HD = 64
D = 768
FF = 3072
LEN = 512
SEQS = 24
TOKENS = 12288


def draw_segment_ids(key, part):
    split_key, label_key = jax.random.split(jax.random.fold_in(key, 11))
    split_rows = jax.random.randint(split_key, (SEQS,), LEN // 64, 3 * LEN // 64 + 1)
    labels = 2 * jax.random.permutation(label_key, SEQS).astype(jnp.int32)
    places = jnp.arange(LEN)
    second = (places[None, :] >= 16 * split_rows[:, None]).astype(jnp.int32)
    return (labels[:, None] + second).reshape(SEQS * LEN).astype(jnp.int32)


def block_scale(rng, extent, cuts, low, largest):
    level = 1.0
    for axis_at, blocks in cuts:
        heights = jax.random.uniform(jax.random.fold_in(jax.random.fold_in(rng, 6), axis_at), (blocks,), jnp.float32, low / len(cuts), largest / len(cuts))
        level = level * jnp.repeat(jnp.exp(heights), extent[axis_at] // blocks).reshape((-1,) + (1,) * (len(extent) - 1 - axis_at))
    return level


def noise(rng, dims, spread, limit, cuts=(), held_as=jnp.bfloat16):
    loudness = block_scale(rng, dims, cuts, -0.22, 0.18) if cuts else 1.0
    drawn = jax.random.normal(rng, dims, jnp.float32) * spread * loudness
    return jnp.minimum(jnp.maximum(drawn, -limit), limit).astype(held_as)


def setup_inputs(seed: int = 0) -> dict:
    splits = jax.random.split(jax.random.key(seed), 16)
    tokens = noise(splits[0], (TOKENS, D), 1.0, 6.0, ((0, 8),))
    segment_ids = draw_segment_ids(jax.random.fold_in(splits[15], 71), 0)
    first_gain = jnp.clip(1.0 + 0.15 * jax.random.normal(splits[2], (D,), jnp.float32), 0.25, 1.75).astype(jnp.bfloat16)
    first_shift = noise(splits[3], (D,), 0.3, 3.0)
    qkv_weight = noise(splits[4], (D, 3, D), D ** -0.5, 0.21875, ((2, 4),))
    qv_bias = noise(splits[5], (2, HEADS, HD), 0.5, 3.0, ((1, 4),))
    proj_weight = noise(splits[6], (D, D), (D // 32) ** -0.5, 1.25, ((0, 4),))
    proj_bias = noise(splits[7], (D,), 0.5, 3.0)
    second_gain = jnp.clip(1.0 + 0.15 * jax.random.normal(splits[8], (D,), jnp.float32), 0.25, 1.75).astype(jnp.bfloat16)
    second_shift = noise(splits[9], (D,), 0.3, 3.0)
    up_weight = noise(splits[10], (D, FF), D ** -0.5, 0.21875, ((1, 4),))
    up_bias = noise(splits[11], (FF // 64, 64), 0.5, 3.0, ((0, 4),))
    down_weight = noise(splits[12], (FF, D), FF ** -0.5, 0.109375, ((0, 4),))
    down_bias = noise(splits[13], (D,), 0.5, 3.0)
    cotangent = noise(splits[14], (TOKENS, D), 1.0, 6.0, ((0, 8),))
    return dict(tokens=tokens, segment_ids=segment_ids, first_gain=first_gain, first_shift=first_shift, qkv_weight=qkv_weight, qv_bias=qv_bias, proj_weight=proj_weight, proj_bias=proj_bias, second_gain=second_gain, second_shift=second_shift, up_weight=up_weight, up_bias=up_bias, down_weight=down_weight, down_bias=down_bias, cotangent=cotangent)


EPS = 1e-06
SCALE = 0.125
NEGATIVE = -1e+30
HIGHEST = lax.Precision.HIGHEST

@jax.custom_vjp
def low(v):
    return lax.optimization_barrier(v.astype(jnp.bfloat16)).astype(jnp.float32)

@jax.custom_vjp
def low_back(v):
    return v

def low_keep(v):
    return (low(v), None)

def low_pass(kept, grad):
    return (grad,)

def back_keep(v):
    return (v, None)

def back_low(kept, grad):
    return (low(grad),)
low.defvjp(low_keep, low_pass)
low_back.defvjp(back_keep, back_low)

def layer_norm(values, gain, shift):
    centre = values - lax.optimization_barrier(jnp.mean(values, axis=-1, keepdims=True))
    variance = lax.optimization_barrier(jnp.mean(centre * centre, axis=-1, keepdims=True))
    return centre * lax.rsqrt(variance + EPS) * gain + shift

def exact_gelu(values):
    return jax.nn.gelu(values, approximate=False)

def block(rows, labels, first_gain, first_shift, qkv_weight, qv_bias, proj_weight, proj_bias, second_gain, second_shift, up_weight, up_bias, down_weight, down_bias):
    count = rows.shape[0] // LEN
    width = rows.shape[1]
    heads = qv_bias.shape[1]
    head_size = qv_bias.shape[2]
    normed1 = low(layer_norm(rows, first_gain, first_shift))
    projected = jnp.einsum('nd,dce->nce', normed1, qkv_weight, precision=HIGHEST)
    query_bias = qv_bias[0].reshape(width)
    bias_rows = jnp.stack([query_bias, jnp.zeros_like(query_bias), qv_bias[1].reshape(width)])
    triple = low(low_back(projected + bias_rows)).reshape(count, LEN, 3, heads, head_size)
    query = triple[:, :, 0]
    keys = triple[:, :, 1]
    values = triple[:, :, 2]
    scores = low_back(SCALE * jnp.einsum('gqhe,gkhe->ghqk', query, keys, precision=HIGHEST))
    image_ids = labels.reshape(count, LEN)
    same = image_ids[:, None, :, None] == image_ids[:, None, None, :]
    scores = jnp.where(same, scores, NEGATIVE)
    probs = jax.nn.softmax(scores, axis=-1)
    mixed = jnp.einsum('ghqk,gkhe->gqhe', low(probs), values, precision=HIGHEST)
    mixed = low(low_back(mixed.reshape(count * LEN, width)))
    attended = low_back(jnp.dot(mixed, proj_weight, precision=HIGHEST))
    middle = rows + attended + proj_bias
    normed2 = low(layer_norm(middle, second_gain, second_shift))
    hidden_pre = low_back(jnp.dot(normed2, up_weight, precision=HIGHEST) + up_bias.reshape(-1))
    hidden = low(exact_gelu(hidden_pre))
    fed = low_back(jnp.dot(hidden, down_weight, precision=HIGHEST))
    return middle + fed + down_bias

def reference(tokens, segment_ids, first_gain, first_shift, qkv_weight, qv_bias, proj_weight, proj_bias, second_gain, second_shift, up_weight, up_bias, down_weight, down_bias, cotangent):
    width = tokens.shape[1]
    seqs_all = tokens.shape[0] // LEN
    group = math.gcd(seqs_all, 8)
    blocks = seqs_all // group
    labels = segment_ids.reshape(blocks, group * LEN)
    params = tuple((p.astype(jnp.float32) for p in (first_gain, first_shift, qkv_weight, qv_bias, proj_weight, proj_bias, second_gain, second_shift, up_weight, up_bias, down_weight, down_bias)))
    saved_block = jax.checkpoint(block)

    def forward(inputs, *weights):
        grouped = inputs.reshape(blocks, group * LEN, width)

        def step(carry, items):
            return (carry, saved_block(items[0], items[1], *weights))
        carry, outputs = lax.scan(step, jnp.zeros((), jnp.float32), (grouped, labels))
        return outputs.reshape(blocks * group * LEN, width)
    result, pull = jax.vjp(forward, tokens.astype(jnp.float32), *params)
    grads = pull(cotangent.astype(jnp.float32))
    return (result.astype(jnp.bfloat16), grads[0].astype(jnp.bfloat16), grads[1], grads[2], grads[3], grads[4], grads[5], grads[6], grads[7], grads[8], grads[9], grads[10], grads[11], grads[12])
```

```python
import math

import jax
import jax.numpy as jnp
from jax import lax
from jax.experimental import pallas as pl
from jax.experimental.pallas import tpu as pltpu
from jax.sharding import PartitionSpec as P

LEN = 512
EPS = 1e-06
SCALE = 0.125
NEGATIVE = -1e30
LOG2E = math.log2(math.e)


def normalize(values):
    centre = values - jnp.mean(values, axis=-1, keepdims=True)
    inverse = lax.rsqrt(jnp.mean(centre * centre, axis=-1, keepdims=True) + EPS)
    return (centre * inverse, inverse)


def norm_backward(grad_normed, unit, inverse, gain):
    scaled = grad_normed * gain
    return inverse * (
        scaled
        - jnp.mean(scaled, axis=-1, keepdims=True)
        - unit * jnp.mean(scaled * unit, axis=-1, keepdims=True)
    )


def over_x(values):
    return lax.ppermute(values, "mp", [(i, i ^ 2) for i in range(4)])


def over_core(values):
    return lax.ppermute(values, "mp", [(i, i ^ 1) for i in range(4)])


def narrow_kernel(wide, low):
    low[...] = wide[...].astype(jnp.bfloat16)


def narrow(wide):
    rows, width = wide.shape
    block = pl.BlockSpec((rows // 2, width), lambda i: (i, 0))
    return pl.pallas_call(
        narrow_kernel,
        grid=(2,),
        in_specs=[block],
        out_specs=block,
        out_shape=jax.ShapeDtypeStruct((rows, width), jnp.bfloat16),
        cost_estimate=pl.CostEstimate(
            flops=rows * width, bytes_accessed=rows * width * 6, transcendentals=0
        ),
        name="narrow",
    )(wide)


def send_low(mover, low):
    return narrow(mover(low.astype(jnp.float32)))


def over_dp(values, count, bit):
    return lax.ppermute(values, "dp", [(i, i ^ (1 << bit)) for i in range(count)])


def scatter_dp(partial, count):
    here = lax.axis_index("dp")
    width = partial.shape[1]
    block = partial.shape[0] // count
    held = partial.reshape(count, block, width)
    for bit in range(count.bit_length() - 1):
        mine = (here >> bit) & 1
        split = held.reshape(held.shape[0] // 2, 2, block, width)
        keep = lax.dynamic_index_in_dim(split, mine, 1, keepdims=False)
        give = lax.dynamic_index_in_dim(split, 1 - mine, 1, keepdims=False)
        held = keep + over_dp(give, count, bit)
    return held[0]


def sum_dp(values, count):
    for bit in range(count.bit_length() - 1):
        values = values + over_dp(values, count, bit)
    return values


def dot_last(left, right):
    return lax.dot_general(
        left, right, (((1,), (1,)), ((), ())), preferred_element_type=jnp.float32
    )


def dot(left, right):
    return jnp.dot(left, right, preferred_element_type=jnp.float32)


def low_head(block):
    lanes = lax.broadcasted_iota(jnp.int32, block.shape, 1)
    return lanes < block.shape[1] // 2


def head_of(block, head):
    wide = block.astype(jnp.float32)
    first = low_head(block)
    zero = jnp.zeros_like(wide)
    kept = jnp.where(first, wide, zero) if head == 0 else jnp.where(first, zero, wide)
    return kept.astype(jnp.bfloat16)


def attend_kernel(key_ids, query_ids, query, keys, values, mixed, log_total):
    same = key_ids[...] == query_ids[0]
    turned = values[...].astype(jnp.float32).T.astype(jnp.bfloat16)
    size = turned.shape[0] // 2
    parts = []
    for head in range(2):
        raw = dot_last(head_of(keys[...], head), query[...])
        raw = jnp.where(same, raw, NEGATIVE)
        top = jnp.max(raw, axis=0, keepdims=True)
        expo = jnp.exp2((raw - top) * (SCALE * LOG2E))
        total = jnp.sum(expo, axis=0, keepdims=True)
        probs = (expo * (1.0 / total)).astype(jnp.bfloat16)
        parts.append(dot(turned[head * size : (head + 1) * size], probs))
        log_total[0, 0, head : head + 1, :] = top * (SCALE * LOG2E) + jnp.log2(total)
    mixed[...] = jnp.concatenate(parts, axis=0).T.astype(jnp.bfloat16)


def attend_back_kernel(key_ids, query_ids, query, keys, values, grad_mixed, log_total, grads):
    same = key_ids[...] == query_ids[0]
    turned = keys[...].astype(jnp.float32).T.astype(jnp.bfloat16)
    size = turned.shape[0] // 2
    grad_query = []
    grad_keys = []
    grad_values = []
    for head in range(2):
        raw = dot_last(head_of(keys[...], head), query[...])
        scaled = jnp.where(same, raw * (SCALE * LOG2E), NEGATIVE)
        probs = jnp.exp2(scaled - log_total[0, 0, head : head + 1, :])
        grad_probs = dot_last(head_of(values[...], head), grad_mixed[...])
        inner = jnp.sum(probs * grad_probs, axis=0, keepdims=True)
        grad_scores = (probs * (grad_probs - inner)).astype(jnp.bfloat16)
        grad_query.append(dot(turned[head * size : (head + 1) * size], grad_scores))
        grad_keys.append(dot(grad_scores, query[...]))
        grad_values.append(dot(probs.astype(jnp.bfloat16), grad_mixed[...]))
    first = low_head(query)
    grads[0] = (SCALE * jnp.concatenate(grad_query, axis=0).T).astype(jnp.bfloat16)
    grads[1] = (SCALE * jnp.where(first, grad_keys[0], grad_keys[1])).astype(jnp.bfloat16)
    grads[2] = jnp.where(first, grad_values[0], grad_values[1]).astype(jnp.bfloat16)


def attend(triple, key_ids, query_ids):
    rows = triple.shape[0]
    width = triple.shape[1] // 3
    pairs = width // 128
    count = rows // LEN

    def part(index):
        return pl.BlockSpec((LEN, 128), lambda s, p: (s, index * pairs + p))

    return pl.pallas_call(
        attend_kernel,
        grid=(count, pairs),
        in_specs=[
            pl.BlockSpec((LEN, 1), lambda s, p: (s, 0)),
            pl.BlockSpec((1, 1, LEN), lambda s, p: (s, 0, 0)),
            part(0),
            part(1),
            part(2),
        ],
        out_specs=[
            pl.BlockSpec((LEN, 128), lambda s, p: (s, p)),
            pl.BlockSpec((1, 1, 2, LEN), lambda s, p: (s, p, 0, 0)),
        ],
        out_shape=[
            jax.ShapeDtypeStruct((rows, width), jnp.bfloat16),
            jax.ShapeDtypeStruct((count, pairs, 2, LEN), jnp.float32),
        ],
        cost_estimate=pl.CostEstimate(
            flops=rows * LEN * width * 8, bytes_accessed=rows * width * 12, transcendentals=0
        ),
        name="attend",
    )(key_ids, query_ids, triple, triple, triple)


def attend_back(triple, key_ids, query_ids, grad_mixed, log_total, seq):
    width = triple.shape[1] // 3
    pairs = width // 128

    def part(index):
        return pl.BlockSpec((LEN, 128), lambda p: (seq, index * pairs + p))

    return pl.pallas_call(
        attend_back_kernel,
        grid=(pairs,),
        in_specs=[
            pl.BlockSpec((LEN, 1), lambda p: (seq, 0)),
            pl.BlockSpec((1, 1, LEN), lambda p: (seq, 0, 0)),
            part(0),
            part(1),
            part(2),
            pl.BlockSpec((LEN, 128), lambda p: (0, p)),
            pl.BlockSpec((1, 1, 2, LEN), lambda p: (seq, p, 0, 0)),
        ],
        out_specs=pl.BlockSpec((3, LEN, 128), lambda p: (0, 0, p)),
        out_shape=jax.ShapeDtypeStruct((3, LEN, width), jnp.bfloat16),
        cost_estimate=pl.CostEstimate(
            flops=LEN * LEN * width * 20, bytes_accessed=LEN * width * 16, transcendentals=0
        ),
        name="attend_back",
    )(key_ids, query_ids, triple, triple, triple, grad_mixed, log_total)


def gelu_parts(values):
    cdf = 0.5 * (1.0 + lax.erf(values * (0.5**0.5)))
    density = jnp.exp(-0.5 * values * values) * ((2.0 * math.pi) ** -0.5)
    return (values * cdf, cdf + values * density)


def shards(
    count_dp,
    tokens,
    segment_ids,
    first_gain,
    first_shift,
    qkv_weight,
    qv_bias,
    proj_weight,
    proj_bias,
    second_gain,
    second_shift,
    up_weight,
    up_bias,
    down_weight,
    down_bias,
    cotangent,
):
    rows, model = tokens.shape
    heads_here = qv_bias.shape[1]
    head_size = qv_bias.shape[2]
    local = heads_here * head_size
    count = rows // LEN
    half = LEN // 2
    odd = lax.axis_index("mp") % 2 == 1

    def orient(values):
        split = values.reshape((count, 2, half) + values.shape[1:])
        return jnp.where(odd, split[:, ::-1], split).reshape(values.shape)

    def mirror(values):
        split = values.reshape((-1, 2, half) + values.shape[1:])
        return split[:, ::-1].reshape(values.shape)

    def seq_rows(values, seq):
        return values[seq * LEN : (seq + 1) * LEN]

    own_qkv = qkv_weight.reshape(model, 3, local)
    far_qkv = send_low(over_x, own_qkv.reshape(model, 3 * local)).reshape(model, 3, local)
    far_bias = over_x(qv_bias.reshape(2, local).astype(jnp.float32))
    far_proj = send_low(over_x, proj_weight)
    qkv_six = jnp.concatenate([own_qkv, far_qkv], axis=2).reshape(model, 6 * local)
    own_bias = qv_bias.reshape(2, local)
    bias_six = jnp.concatenate([own_bias.astype(jnp.float32), far_bias], axis=1)
    bias_row = jnp.concatenate(
        [bias_six[0], jnp.zeros_like(bias_six[0]), bias_six[1]], axis=0
    )
    proj_six = jnp.concatenate([proj_weight, far_proj], axis=0)
    proj_other = send_low(over_core, proj_six)

    gain_one = first_gain.astype(jnp.float32)
    gain_two = second_gain.astype(jnp.float32)
    tokens = orient(tokens)
    cotangent = orient(cotangent)
    image_ids = orient(segment_ids)
    key_ids = image_ids.reshape(rows, 1)
    query_ids = image_ids.reshape(count, 1, LEN)

    inputs = tokens.astype(jnp.float32)
    first_unit, first_inverse = normalize(inputs)
    normed1 = (first_unit * gain_one + first_shift.astype(jnp.float32)).astype(jnp.bfloat16)
    triple = (dot(normed1, qkv_six) + bias_row).astype(jnp.bfloat16)
    mixed, log_total = attend(triple, key_ids, query_ids)
    mixed_other = mirror(send_low(over_core, mixed))
    attended = dot(
        jnp.concatenate([mixed, mixed_other], axis=1),
        jnp.concatenate([proj_six, proj_other], axis=0),
    )
    middle = inputs + attended + proj_bias.astype(jnp.float32)
    second_unit, second_inverse = normalize(middle)
    normed2 = (second_unit * gain_two + second_shift.astype(jnp.float32)).astype(jnp.bfloat16)

    up_flat = up_bias.reshape(-1).astype(jnp.float32)
    hidden_pre = dot(normed2, up_weight) + up_flat
    activated, slope = gelu_parts(hidden_pre)
    hidden = activated.astype(jnp.bfloat16)
    grad_pre = (dot_last(cotangent, down_weight) * slope).astype(jnp.bfloat16)

    def reduce_begin(low, weight, contract, seq):
        block = seq_rows(low, seq)
        give = contract(block[half:], weight)
        keep = contract(block[:half], weight)
        return keep + over_core(give)

    def reduce_end(chip_sum, far):
        total = chip_sum + far
        return jnp.concatenate([total, over_core(total)], axis=0)

    back_chip = [reduce_begin(grad_pre, up_weight, dot_last, s) for s in range(count)]
    back_far = [over_x(v) for v in back_chip]
    grad_normed2 = [reduce_end(a, b) for a, b in zip(back_chip, back_far)]
    fed_chip = [reduce_begin(hidden, down_weight, dot, s) for s in range(count)]
    fed_chip, back_far = lax.optimization_barrier((fed_chip, back_far))
    fed = [reduce_end(v, over_x(v)) for v in fed_chip]
    fed = jnp.concatenate(fed, axis=0)
    layer_output = (middle + fed + down_bias.astype(jnp.float32)).astype(jnp.bfloat16)

    grad_out = cotangent.astype(jnp.float32)
    down_bias_grad = jnp.sum(grad_out, axis=0)
    up_bias_grad = jnp.sum(grad_pre, axis=0, dtype=jnp.float32)

    def dot_first(left, right):
        return lax.dot_general(
            left, right, (((0,), (0,)), ((), ())), preferred_element_type=jnp.float32
        )

    down_part = scatter_dp(dot_first(cotangent, hidden), count_dp)
    up_part = scatter_dp(dot_first(normed2, grad_pre), count_dp)

    second_gain_grad = 0.0
    second_shift_grad = 0.0
    proj_bias_grad = 0.0
    grad_middle = []
    middle_low = []
    grad_triple = []
    grad_normed1 = []
    qkv_parts = qkv_six.reshape(model, 3, 2 * local)
    for seq in range(count):
        unit = seq_rows(second_unit, seq)
        normed_grad = grad_normed2[seq]
        second_gain_grad = second_gain_grad + jnp.sum(normed_grad * unit, axis=0)
        second_shift_grad = second_shift_grad + jnp.sum(normed_grad, axis=0)
        piece = seq_rows(grad_out, seq) + norm_backward(
            normed_grad, unit, seq_rows(second_inverse, seq), gain_two
        )
        proj_bias_grad = proj_bias_grad + jnp.sum(piece, axis=0)
        low = piece.astype(jnp.bfloat16)
        grad_middle.append(piece)
        middle_low.append(low)
        grad_mixed = dot_last(low, proj_six).astype(jnp.bfloat16)
        grads = attend_back(triple, key_ids, query_ids, grad_mixed, log_total, seq)
        grad_triple.append(grads)
        partial = (
            dot_last(grads[0], qkv_parts[:, 0])
            + dot_last(grads[1], qkv_parts[:, 1])
            + dot_last(grads[2], qkv_parts[:, 2])
        )
        grad_normed1.append(partial + mirror(over_core(partial)))
    grad_rows = jnp.concatenate(grad_triple, axis=1)[:, :, :local]
    low_rows = jnp.concatenate(middle_low, axis=0)
    proj_part = scatter_dp(dot_first(low_rows, mixed[:, :local]), count_dp)
    qkv_grad = jnp.concatenate([dot_first(normed1, grad_rows[j]) for j in range(3)], axis=1)
    qkv_part = scatter_dp(qkv_grad, count_dp)
    qv_bias_grad = jnp.concatenate(
        [
            jnp.sum(grad_rows[0], axis=0, dtype=jnp.float32),
            jnp.sum(grad_rows[2], axis=0, dtype=jnp.float32),
        ]
    )
    grad_normed1 = jnp.concatenate(grad_normed1, axis=0)
    first_gain_grad = jnp.sum(grad_normed1 * first_unit, axis=0)
    first_shift_grad = jnp.sum(grad_normed1, axis=0)
    input_grad = (
        jnp.concatenate(grad_middle, axis=0)
        + norm_backward(grad_normed1, first_unit, first_inverse, gain_one)
    ).astype(jnp.bfloat16)

    flat = jnp.concatenate(
        [
            first_gain_grad,
            first_shift_grad,
            proj_bias_grad,
            second_gain_grad,
            second_shift_grad,
            down_bias_grad,
            up_bias_grad,
            qv_bias_grad,
        ]
    )
    sums = sum_dp(flat, count_dp)
    here = lax.axis_index("dp")

    def share(values, axis):
        size = values.shape[axis] // count_dp
        return lax.dynamic_slice_in_dim(values, here * size, size, axis)

    vectors = share(sums[: 6 * model].reshape(6, model), 1)
    up_bias_sum = sums[6 * model : 6 * model + up_flat.shape[0]].reshape(up_bias.shape)
    qv_sum = sums[6 * model + up_flat.shape[0] :].reshape(qv_bias.shape)
    return (
        orient(layer_output),
        orient(input_grad),
        vectors[0],
        vectors[1],
        qkv_part.reshape(-1, 3, local),
        share(qv_sum, 2),
        proj_part.T,
        vectors[2],
        vectors[3],
        vectors[4],
        up_part,
        share(up_bias_sum, 1),
        down_part.T,
        vectors[5],
    )


def solution(mesh):
    count_dp = mesh.shape["dp"]

    def whole(*args):
        return shards(count_dp, *args)

    in_specs = (
        P("dp", None),
        P("dp"),
        P(),
        P(),
        P(None, None, "mp"),
        P(None, "mp", None),
        P("mp", None),
        P(),
        P(),
        P(),
        P(None, "mp"),
        P("mp", None),
        P("mp", None),
        P(),
        P("dp", None),
    )
    out_specs = (
        P("dp", None),
        P("dp", None),
        P("dp"),
        P("dp"),
        P("dp", None, "mp"),
        P(None, "mp", "dp"),
        P("mp", "dp"),
        P("dp"),
        P("dp"),
        P("dp"),
        P("dp", "mp"),
        P("mp", "dp"),
        P("mp", "dp"),
        P("dp"),
    )
    return jax.shard_map(whole, mesh=mesh, in_specs=in_specs, out_specs=out_specs, check_vma=False)
```

```python
import math

import jax
import jax.numpy as jnp
from jax import lax
from jax.experimental import pallas as pl
from jax.experimental.pallas import tpu as pltpu
from jax.sharding import PartitionSpec as P

LEN = 512
HALF = LEN // 2
EPS = 1e-06
SCALE = 0.125
NEGATIVE = -1e30
LOG2E = math.log2(math.e)
LOW = jnp.bfloat16
WIDE = jnp.float32


def normalize(values):
    centre = values - jnp.mean(values, axis=-1, keepdims=True)
    inverse = lax.rsqrt(jnp.mean(centre * centre, axis=-1, keepdims=True) + EPS)
    return (centre * inverse, inverse)


def norm_backward(grad_normed, unit, inverse, gain):
    scaled = grad_normed * gain
    return inverse * (
        scaled
        - jnp.mean(scaled, axis=-1, keepdims=True)
        - unit * jnp.mean(scaled * unit, axis=-1, keepdims=True)
    )


def over_x(values):
    return lax.ppermute(values, "mp", [(i, i ^ 2) for i in range(4)])


def over_core(values):
    return lax.ppermute(values, "mp", [(i, i ^ 1) for i in range(4)])


def over_dp(values, count, bit):
    return lax.ppermute(values, "dp", [(i, i ^ (1 << bit)) for i in range(count)])


def scatter_dp(partial, count):
    here = lax.axis_index("dp")
    width = partial.shape[1]
    block = partial.shape[0] // count
    held = lax.optimization_barrier(partial).reshape(count, block, width)
    for bit in range(count.bit_length() - 1):
        mine = (here >> bit) & 1
        split = held.reshape(held.shape[0] // 2, 2, block, width)
        keep = lax.dynamic_index_in_dim(split, mine, 1, keepdims=False)
        give = lax.dynamic_index_in_dim(split, 1 - mine, 1, keepdims=False)
        got = over_dp(give, count, bit)
        held = keep + got
    return held[0]


def sum_dp(values, count):
    for bit in range(count.bit_length() - 1):
        values = values + over_dp(values, count, bit)
    return values


def dot_last(left, right):
    return lax.dot_general(
        left, right, (((1,), (1,)), ((), ())), preferred_element_type=WIDE
    )


def dot_first(left, right):
    return lax.dot_general(
        left, right, (((0,), (0,)), ((), ())), preferred_element_type=WIDE
    )


def dot(left, right):
    return jnp.dot(left, right, preferred_element_type=WIDE)


def call(kernel, grid, in_specs, out_specs, out_shape, args, flops, prefetch=None, shared=()):
    args = list(args)
    in_specs = list(in_specs)
    aliases = {}
    lead = 0 if prefetch is None else 1
    inputs = len(args)
    for index, buffer in shared:
        if buffer is not None:
            aliases[lead + len(args)] = index
            args.append(buffer)
            in_specs.append(pl.BlockSpec(memory_space=pl.ANY))
    extra = len(args) - inputs

    def body(*refs):
        refs = refs[lead:]
        kernel(*refs[:inputs], *refs[inputs + extra :])

    spec = pltpu.PrefetchScalarGridSpec(
        num_scalar_prefetch=lead, grid=grid, in_specs=in_specs, out_specs=out_specs
    )
    moved = sum(math.prod(a.shape) * a.dtype.itemsize for a in args[:inputs])
    return pl.pallas_call(
        body,
        grid_spec=spec,
        out_shape=out_shape,
        input_output_aliases=aliases,
        cost_estimate=pl.CostEstimate(
            flops=flops, bytes_accessed=moved, transcendentals=0
        ),
    )(*(() if prefetch is None else (prefetch,)), *args)


def whole(shape):
    return pl.BlockSpec(shape, lambda *_: (0,) * len(shape))


def row_sum(values):
    return jnp.sum(values, axis=0, keepdims=True)


def tally(step, sums, rows):
    @pl.when(step == 0)
    def _():
        sums[...] = jnp.zeros_like(sums)

    for index, row in enumerate(rows):
        sums[index : index + 1, :] += row


def blend_kernel(own, far, out):
    out[0, 0] = own[0, :128]
    out[1, 0, :64] = own[0, 128:]
    out[1, 0, 64:] = far[0, :64].astype(LOW)
    out[2, 0] = far[0, 64:].astype(LOW)


def pack_kernel(first, second, third, fourth, out):
    rows = first.shape[0]
    for index, part in enumerate((first, second, third, fourth)):
        out[index * rows : (index + 1) * rows, :] = part[...].astype(LOW)


def front_kernel(tokens, gain, shift, weight, bias, normed, triple):
    unit, _ = normalize(tokens[...].astype(WIDE))
    low = (unit * gain[...] + shift[...]).astype(LOW)
    normed[...] = low
    rows = weight.shape[0] * weight.shape[1]
    triple[...] = (
        dot_last(low, weight[...].reshape(rows, weight.shape[2])) + bias[...]
    ).astype(LOW)


def low_head(block):
    lanes = lax.broadcasted_iota(jnp.int32, block.shape, 1)
    return lanes < block.shape[1] // 2


def head_of(block, head):
    wide = block.astype(WIDE)
    first = low_head(block)
    zero = jnp.zeros_like(wide)
    kept = jnp.where(first, wide, zero) if head == 0 else jnp.where(first, zero, wide)
    return kept.astype(LOW)


def parts_of(block):
    return block[:, :128], block[:, 128:256], block[:, 256:]


def attend_kernel(key_ids, query_ids, triple, mixed, log_total):
    same = key_ids[...] == query_ids[0]
    query, keys, values = parts_of(triple[...])
    turned = values.astype(WIDE).T.astype(LOW)
    size = turned.shape[0] // 2
    parts = []
    for head in range(2):
        raw = dot_last(head_of(keys, head), query)
        raw = jnp.where(same, raw, NEGATIVE)
        top = jnp.max(raw, axis=0, keepdims=True)
        expo = jnp.exp2((raw - top) * (SCALE * LOG2E))
        total = jnp.sum(expo, axis=0, keepdims=True)
        probs = (expo * (1.0 / total)).astype(LOW)
        parts.append(dot(turned[head * size : (head + 1) * size], probs))
        log_total[0, 0, head : head + 1, :] = top * (SCALE * LOG2E) + jnp.log2(total)
    mixed[...] = jnp.concatenate(parts, axis=0).T.astype(LOW).astype(WIDE)


def attend(triple, key_ids, query_ids, start, count):
    pairs = triple.shape[1] // 384
    return call(
        attend_kernel,
        (count, pairs),
        [
            pl.BlockSpec((LEN, 1), lambda s, p: (start + s, 0)),
            pl.BlockSpec((1, 1, LEN), lambda s, p: (start + s, 0, 0)),
            pl.BlockSpec((LEN, 384), lambda s, p: (start + s, p)),
        ],
        [
            pl.BlockSpec((LEN, 128), lambda s, p: (s, p)),
            pl.BlockSpec((1, 1, 2, LEN), lambda s, p: (s, p, 0, 0)),
        ],
        [
            jax.ShapeDtypeStruct((count * LEN, pairs * 128), WIDE),
            jax.ShapeDtypeStruct((count, pairs, 2, LEN), WIDE),
        ],
        (key_ids, query_ids, triple),
        flops=count * pairs * LEN * LEN * 1024,
    )


def attend_back_kernel(
    key_ids,
    query_ids,
    triple_own,
    triple_rest,
    grad_mixed,
    log_own,
    log_rest,
    weight,
    own_pair,
    own_last,
    partial,
    sums,
):
    pair = pl.program_id(0)
    lead = pair == 0
    same = key_ids[...] == query_ids[0]
    block = jnp.where(
        lead, triple_own[...].astype(WIDE), triple_rest[...].astype(WIDE)
    ).astype(LOW)
    log_total = jnp.where(lead, log_own[0, 0], log_rest[0, 0])
    query, keys, values = parts_of(block)
    turned = keys.astype(WIDE).T.astype(LOW)
    size = turned.shape[0] // 2
    grad_query = []
    grad_keys = []
    grad_values = []
    for head in range(2):
        raw = dot_last(head_of(keys, head), query)
        scaled = jnp.where(same, raw * (SCALE * LOG2E), NEGATIVE)
        probs = jnp.exp2(scaled - log_total[head : head + 1, :])
        grad_probs = dot_last(head_of(values, head), grad_mixed[...])
        inner = jnp.sum(probs * grad_probs, axis=0, keepdims=True)
        grad_scores = (probs * (grad_probs - inner)).astype(LOW)
        grad_query.append(dot(turned[head * size : (head + 1) * size], grad_scores))
        grad_keys.append(dot(grad_scores, query))
        grad_values.append(dot(probs.astype(LOW), grad_mixed[...]))
    first = low_head(query)
    grads = jnp.concatenate(
        [
            SCALE * jnp.concatenate(grad_query, axis=0).T,
            SCALE * jnp.where(first, grad_keys[0], grad_keys[1]),
            jnp.where(first, grad_values[0], grad_values[1]),
        ],
        axis=1,
    ).astype(LOW)
    through = dot(grads, weight[...])
    tally(0, sums.at[0], [row_sum(grads.astype(WIDE))])

    @pl.when(lead)
    def _():
        own_pair[...] = grads
        partial[...] = through

    @pl.when(pair == 1)
    def _():
        own_last[...] = jnp.concatenate(
            [part[:, :64].astype(WIDE) for part in parts_of(grads)], axis=1
        ).astype(LOW)

    @pl.when(pair > 0)
    def _():
        partial[...] += through


def attend_back(
    triple_own, triple_rest, key_ids, query_ids, grad_mixed, log_own, log_rest, weight, seq, shared
):
    rows = triple_own.shape[0]
    model = weight.shape[1]
    pairs = weight.shape[0] // 384

    def rest(p):
        return jnp.maximum(p - 1, 0)

    return call(
        attend_back_kernel,
        (pairs,),
        [
            pl.BlockSpec((LEN, 1), lambda p: (seq, 0)),
            pl.BlockSpec((1, 1, LEN), lambda p: (seq, 0, 0)),
            pl.BlockSpec((LEN, 384), lambda p: (seq, 0)),
            pl.BlockSpec((LEN, 384), lambda p: (seq, rest(p))),
            pl.BlockSpec((LEN, 128), lambda p: (0, p)),
            pl.BlockSpec((1, 1, 2, LEN), lambda p: (seq, 0, 0, 0)),
            pl.BlockSpec((1, 1, 2, LEN), lambda p: (0, rest(p), 0, 0)),
            pl.BlockSpec((384, model), lambda p: (p, 0)),
        ],
        [
            pl.BlockSpec((LEN, 384), lambda p: (seq, 0)),
            pl.BlockSpec((LEN, 192), lambda p: (seq, 0)),
            pl.BlockSpec((LEN, model), lambda p: (0, 0)),
            pl.BlockSpec((1, 8, 384), lambda p: (p, 0, 0)),
        ],
        [
            jax.ShapeDtypeStruct((rows, 384), LOW),
            jax.ShapeDtypeStruct((rows, 192), LOW),
            jax.ShapeDtypeStruct((LEN, model), WIDE),
            jax.ShapeDtypeStruct((pairs, 8, 384), WIDE),
        ],
        (key_ids, query_ids, triple_own, triple_rest, grad_mixed, log_own, log_rest, weight),
        flops=pairs * LEN * LEN * 3328,
        shared=((0, shared[0]), (1, shared[1])),
    )


def gelu_parts(values):
    cdf = 0.5 * (1.0 + lax.erf(values * (0.5**0.5)))
    density = jnp.exp(-0.5 * values * values) * ((2.0 * math.pi) ** -0.5)
    return (values * cdf, cdf + values * density)


def middle_kernel(
    tokens,
    mixed_own,
    mixed_rest,
    other_own,
    other_rest,
    proj,
    proj_bias,
    gain,
    shift,
    up,
    up_bias,
    down,
    cotangent,
    middle,
    normed2,
    hidden,
    grad_pre,
    mixed_kept,
    back_part,
    fed_part,
    sums,
):
    mixed = jnp.concatenate(
        [mixed_own[...], mixed_rest[...], other_own[...], other_rest[...]], axis=1
    ).astype(LOW)
    mixed_kept[...] = mixed[:, :192]
    summed = tokens[...].astype(WIDE) + dot(mixed, proj[...]) + proj_bias[...]
    middle[...] = summed
    unit, _ = normalize(summed)
    normed = (unit * gain[...] + shift[...]).astype(LOW)
    normed2[...] = normed
    activated, slope = gelu_parts(dot(normed, up[...]) + up_bias[...])
    kept = activated.astype(LOW)
    hidden[...] = kept
    grad = (dot_last(cotangent[...], down[...]) * slope).astype(LOW)
    grad_pre[...] = grad
    back_part[0] = dot_last(grad, up[...])
    fed_part[0] = dot(kept, down[...])
    tally(
        pl.program_id(0),
        sums,
        [row_sum(cotangent[...].astype(WIDE)), row_sum(grad.astype(WIDE))],
    )


def back_norm_kernel(
    total, other, is_odd, middle, cotangent, gain, proj, grad_middle, low, grad_mixed, sums
):
    own = pl.program_id(0) == is_odd[0]
    normed_grad = jnp.where(own, total[...], other[...])
    unit, inverse = normalize(middle[...])
    piece = cotangent[...].astype(WIDE) + norm_backward(normed_grad, unit, inverse, gain[...])
    grad_middle[...] = piece
    rounded = piece.astype(LOW)
    low[...] = rounded
    grad_mixed[...] = dot_last(rounded, proj[...]).astype(LOW)
    tally(
        pl.program_id(0),
        sums,
        [row_sum(normed_grad * unit), row_sum(normed_grad), row_sum(piece)],
    )


def final_kernel(partial, other, tokens, grad_middle, gain, input_grad, sums):
    normed_grad = partial[...] + other[...]
    unit, inverse = normalize(tokens[...].astype(WIDE))
    input_grad[...] = (
        grad_middle[...] + norm_backward(normed_grad, unit, inverse, gain[...])
    ).astype(LOW)
    tally(pl.program_id(0), sums, [row_sum(normed_grad * unit), row_sum(normed_grad)])


def output_kernel(total, other, is_odd, middle, bias, out):
    own = pl.program_id(0) == is_odd[0]
    fed = jnp.where(own, total[...], other[...])
    out[...] = (middle[...] + fed + bias[...]).astype(LOW)


def shards(
    count_dp,
    tokens,
    segment_ids,
    first_gain,
    first_shift,
    qkv_weight,
    qv_bias,
    proj_weight,
    proj_bias,
    second_gain,
    second_shift,
    up_weight,
    up_bias,
    down_weight,
    down_bias,
    cotangent,
):
    rows, model = tokens.shape
    local = qv_bias.shape[1] * qv_bias.shape[2]
    hidden_size = up_weight.shape[1]
    count = rows // LEN
    odd = (lax.axis_index("mp") % 2).astype(jnp.int32).reshape(1)

    def row(values):
        return values.astype(WIDE).reshape(1, -1)

    def seq_half(width, seq):
        return pl.BlockSpec((HALF, width), lambda i: (2 * seq + i, 0))

    def half(width):
        return pl.BlockSpec((HALF, width), lambda i: (i, 0))

    own_rows = jnp.transpose(qkv_weight, (1, 2, 0))
    own_bias = qv_bias.reshape(2, local).astype(WIDE)
    far_bias = over_x(own_bias)
    far_rows = over_x(own_rows.reshape(3 * local, model).astype(WIDE))
    proj_wide = proj_weight.astype(WIDE)
    far_proj = over_x(proj_wide)
    core_proj = over_core(proj_wide)
    core_far_proj = over_core(far_proj)

    gain_one = row(first_gain)
    gain_two = row(second_gain)
    key_ids = segment_ids.reshape(rows, 1)
    query_ids = segment_ids.reshape(count, 1, LEN)
    none = jnp.zeros((128,), WIDE)
    bias_own = row(jnp.concatenate([own_bias[0, :128], none, own_bias[1, :128]]))
    bias_rest = row(
        jnp.concatenate(
            [
                own_bias[0, 128:],
                far_bias[0, :64],
                none,
                own_bias[1, 128:],
                far_bias[1, :64],
                far_bias[0, 64:],
                none,
                far_bias[1, 64:],
            ]
        )
    )

    normed1, triple_own = call(
        front_kernel,
        (2 * count,),
        [
            half(model),
            whole((1, model)),
            whole((1, model)),
            whole((3, 128, model)),
            whole((1, 384)),
        ],
        [half(model), half(384)],
        [jax.ShapeDtypeStruct((rows, model), LOW), jax.ShapeDtypeStruct((rows, 384), LOW)],
        (tokens, gain_one, row(first_shift), own_rows, bias_own),
        flops=rows * model * 800,
    )
    mixed_own, log_own = attend(triple_own, key_ids, query_ids, 0, count)
    other_own = over_core(mixed_own)

    weight_six = call(
        blend_kernel,
        (3,),
        [pl.BlockSpec((1, local, model), lambda j: (j, 0, 0))] * 2,
        pl.BlockSpec((3, 1, 128, model), lambda j: (0, j, 0, 0)),
        jax.ShapeDtypeStruct((3, 3, 128, model), LOW),
        (own_rows, far_rows.reshape(3, local, model)),
        flops=6 * local * model,
    ).reshape(6 * local, model)
    triple_rest = (dot_last(normed1, weight_six[384:]) + bias_rest).astype(LOW)
    proj_all = call(
        pack_kernel,
        (1,),
        [whole((local, model))] * 4,
        whole((4 * local, model)),
        jax.ShapeDtypeStruct((4 * local, model), LOW),
        (proj_weight, far_proj, core_proj, core_far_proj),
        flops=4 * local * model,
    )

    def picked(width, seq):
        return pl.BlockSpec(
            (HALF, width), lambda i, is_odd: (2 * seq + (i + 1 + is_odd[0]) % 2, 0)
        )

    def piece(width):
        return pl.BlockSpec((1, HALF, width), lambda i, is_odd: (i, 0, 0))

    attended = []
    for seq in range(count):
        mixed_rest, log_rest = attend(triple_rest, key_ids, query_ids, seq, 1)
        attended.append((mixed_rest, log_rest, over_core(mixed_rest)))

    kept = [None] * 4
    middles = []
    mlp_sums = []
    back_chip = []
    fed_chip = []
    for seq in range(count):
        mixed_rest, _, other_rest = attended[seq]
        middle, *kept, back_part, fed_part, sums = call(
            middle_kernel,
            (2,),
            [
                picked(model, seq),
                picked(128, seq),
                picked(256, 0),
                picked(128, seq),
                picked(256, 0),
                whole((model, model)),
                whole((1, model)),
                whole((1, model)),
                whole((1, model)),
                whole((model, hidden_size)),
                whole((1, hidden_size)),
                whole((hidden_size, model)),
                picked(model, seq),
            ],
            [
                picked(model, 0),
                picked(model, seq),
                picked(hidden_size, seq),
                picked(hidden_size, seq),
                picked(local, seq),
                piece(model),
                piece(model),
                whole((8, model)),
            ],
            [
                jax.ShapeDtypeStruct((LEN, model), WIDE),
                jax.ShapeDtypeStruct((rows, model), LOW),
                jax.ShapeDtypeStruct((rows, hidden_size), LOW),
                jax.ShapeDtypeStruct((rows, hidden_size), LOW),
                jax.ShapeDtypeStruct((rows, local), LOW),
                jax.ShapeDtypeStruct((2, HALF, model), WIDE),
                jax.ShapeDtypeStruct((2, HALF, model), WIDE),
                jax.ShapeDtypeStruct((8, model), WIDE),
            ],
            (
                tokens,
                mixed_own,
                mixed_rest,
                other_own,
                other_rest,
                proj_all,
                row(proj_bias),
                gain_two,
                row(second_shift),
                up_weight,
                row(up_bias),
                down_weight,
                cotangent,
            ),
            flops=LEN * model * model * 10,
            prefetch=odd,
            shared=tuple((1 + i, kept[i]) for i in range(4)),
        )
        middles.append(middle)
        mlp_sums.append(sums)
        back_chip.append(back_part[1] + over_core(back_part[0]))
        fed_chip.append(fed_part[1] + over_core(fed_part[0]))
    normed2, hidden, grad_pre, mixed_kept = kept

    back_far = []
    for seq in range(count):
        back_far.append(over_x(back_chip[seq]))
    fed_far = []
    for seq in range(count):
        fed_far.append(over_x(fed_chip[seq]))

    down_full = dot_first(cotangent, hidden)
    up_full = dot_first(normed2, grad_pre)
    down_part = scatter_dp(down_full, count_dp)
    up_part = scatter_dp(up_full, count_dp)

    low_rows = None
    own_grads = [None, None]
    input_grad = None
    norm_sums = []
    attend_sums = []
    first_sums = []
    in_smem = pl.BlockSpec(memory_space=pltpu.SMEM)
    for seq in range(count):
        total = back_chip[seq] + back_far[seq]
        other = over_core(total)
        grad_middle, low_rows, grad_mixed, sums = call(
            back_norm_kernel,
            (2,),
            [
                whole((HALF, model)),
                whole((HALF, model)),
                in_smem,
                half(model),
                seq_half(model, seq),
                whole((1, model)),
                whole((2 * local, model)),
            ],
            [half(model), seq_half(model, seq), half(2 * local), whole((8, model))],
            [
                jax.ShapeDtypeStruct((LEN, model), WIDE),
                jax.ShapeDtypeStruct((rows, model), LOW),
                jax.ShapeDtypeStruct((LEN, 2 * local), LOW),
                jax.ShapeDtypeStruct((8, model), WIDE),
            ],
            (total, other, odd, middles[seq], cotangent, gain_two, proj_all),
            flops=LEN * model * local * 8,
            shared=((1, low_rows),),
        )
        norm_sums.append(sums)
        *own_grads, partial, sums = attend_back(
            triple_own,
            triple_rest,
            key_ids,
            query_ids,
            grad_mixed,
            log_own,
            attended[seq][1],
            weight_six,
            seq,
            own_grads,
        )
        attend_sums.append(sums)
        other = over_core(partial)
        input_grad, sums = call(
            final_kernel,
            (2,),
            [
                half(model),
                half(model),
                seq_half(model, seq),
                half(model),
                whole((1, model)),
            ],
            [seq_half(model, seq), whole((8, model))],
            [
                jax.ShapeDtypeStruct((rows, model), LOW),
                jax.ShapeDtypeStruct((8, model), WIDE),
            ],
            (partial, other, tokens, grad_middle, gain_one),
            flops=LEN * model * 40,
            shared=((0, input_grad),),
        )
        first_sums.append(sums)

    proj_full = dot_first(low_rows, mixed_kept)
    proj_part = scatter_dp(proj_full, count_dp)
    pair_full = dot_first(normed1, own_grads[0])
    last_full = dot_first(normed1, own_grads[1])
    pair_part = scatter_dp(pair_full, count_dp)
    last_part = scatter_dp(last_full, count_dp)
    block = pair_part.shape[0]
    qkv_part = jnp.concatenate(
        [pair_part.reshape(block, 3, 128), last_part.reshape(block, 3, 64)], axis=2
    )

    layer_output = None
    for seq in range(count):
        total = fed_chip[seq] + fed_far[seq]
        other = over_core(total)
        layer_output = call(
            output_kernel,
            (2,),
            [
                whole((HALF, model)),
                whole((HALF, model)),
                in_smem,
                half(model),
                whole((1, model)),
            ],
            seq_half(model, seq),
            jax.ShapeDtypeStruct((rows, model), LOW),
            (total, other, odd, middles[seq], row(down_bias)),
            flops=LEN * model * 4,
            shared=((0, layer_output),),
        )

    mlp_sums = sum(mlp_sums)
    norm_sums = sum(norm_sums)
    attend_sums = sum(attend_sums)[:2, 0]
    first_sums = sum(first_sums)
    pair_sums = attend_sums[0].reshape(3, 128)
    last_sums = attend_sums[1].reshape(3, 128)[:, :64]
    qv_sums = jnp.concatenate([pair_sums, last_sums], axis=1)
    flat = jnp.concatenate(
        [
            first_sums[0],
            first_sums[1],
            norm_sums[2],
            norm_sums[0],
            norm_sums[1],
            mlp_sums[0],
            mlp_sums[1],
            qv_sums[0],
            qv_sums[2],
        ]
    )
    sums = sum_dp(flat, count_dp)
    here = lax.axis_index("dp")

    def share(values, axis):
        size = values.shape[axis] // count_dp
        return lax.dynamic_slice_in_dim(values, here * size, size, axis)

    vectors = share(sums[: 6 * model].reshape(6, model), 1)
    up_bias_sum = sums[6 * model : 6 * model + hidden_size].reshape(up_bias.shape)
    qv_sum = sums[6 * model + hidden_size :].reshape(qv_bias.shape)
    return (
        layer_output,
        input_grad,
        vectors[0],
        vectors[1],
        qkv_part,
        share(qv_sum, 2),
        proj_part.T,
        vectors[2],
        vectors[3],
        vectors[4],
        up_part,
        share(up_bias_sum, 1),
        down_part.T,
        vectors[5],
    )


def solution(mesh):
    count_dp = mesh.shape["dp"]

    def layer(*args):
        return shards(count_dp, *args)

    in_specs = (
        P("dp", None),
        P("dp"),
        P(),
        P(),
        P(None, None, "mp"),
        P(None, "mp", None),
        P("mp", None),
        P(),
        P(),
        P(),
        P(None, "mp"),
        P("mp", None),
        P("mp", None),
        P(),
        P("dp", None),
    )
    out_specs = (
        P("dp", None),
        P("dp", None),
        P("dp"),
        P("dp"),
        P("dp", None, "mp"),
        P(None, "mp", "dp"),
        P("mp", "dp"),
        P("dp"),
        P("dp"),
        P("dp"),
        P("dp", "mp"),
        P("mp", "dp"),
        P("mp", "dp"),
        P("dp"),
    )
    return jax.shard_map(layer, mesh=mesh, in_specs=in_specs, out_specs=out_specs, check_vma=False)
```

```python
import functools
import math

import jax
import jax.numpy as jnp
from jax import lax
from jax.experimental import pallas as pl
from jax.experimental.pallas import tpu as pltpu
from jax.sharding import PartitionSpec as P


LEN = 512
HALF = LEN // 2
EPS = 1e-06
SCALE = 0.125
NEGATIVE = -1e30
LOG2E = math.log2(math.e)
LOW = jnp.bfloat16
WIDE = jnp.float32


def normalize(values):
    centre = values - jnp.mean(values, axis=-1, keepdims=True)
    inverse = lax.rsqrt(jnp.mean(centre * centre, axis=-1, keepdims=True) + EPS)
    return (centre * inverse, inverse)


def norm_backward(grad_normed, unit, inverse, gain):
    scaled = grad_normed * gain
    return inverse * (
        scaled
        - jnp.mean(scaled, axis=-1, keepdims=True)
        - unit * jnp.mean(scaled * unit, axis=-1, keepdims=True)
    )


def over_x(values):
    return lax.ppermute(values, "mp", [(i, i ^ 2) for i in range(4)])


def over_core(values):
    return lax.ppermute(values, "mp", [(i, i ^ 1) for i in range(4)])


def over_dp(values, count, bit):
    return lax.ppermute(values, "dp", [(i, i ^ (1 << bit)) for i in range(count)])


def scatter_dp(give, keep, count):
    here = lax.axis_index("dp")
    _, block, width = keep.shape
    got = over_dp(give, count, 0)
    held = keep + got
    for bit in range(1, count.bit_length() - 1):
        mine = (here >> bit) & 1
        split = held.reshape(held.shape[0] // 2, 2, block, width)
        keep = lax.dynamic_index_in_dim(split, mine, 1, keepdims=False)
        give = lax.dynamic_index_in_dim(split, 1 - mine, 1, keepdims=False)
        got = over_dp(give, count, bit)
        held = keep + got
    return held[0]


def sum_dp(values, count):
    for bit in range(count.bit_length() - 1):
        got = over_dp(values, count, bit)
        values = values + got
    return values


def dot_last(left, right):
    return lax.dot_general(
        left, right, (((1,), (1,)), ((), ())), preferred_element_type=WIDE
    )


def dot_first(left, right):
    return lax.dot_general(
        left, right, (((0,), (0,)), ((), ())), preferred_element_type=WIDE
    )


def dot(left, right):
    return jnp.dot(left, right, preferred_element_type=WIDE)


def call(kernel, grid, in_specs, out_specs, out_shape, args, flops, prefetch=None, shared=()):
    args = list(args)
    in_specs = list(in_specs)
    aliases = {}
    lead = 0 if prefetch is None else 1
    inputs = len(args)
    for index, buffer in shared:
        if buffer is not None:
            aliases[lead + len(args)] = index
            args.append(buffer)
            in_specs.append(pl.BlockSpec(memory_space=pl.ANY))
    extra = len(args) - inputs

    def body(*refs):
        refs = refs[lead:]
        kernel(*refs[:inputs], *refs[inputs + extra :])

    spec = pltpu.PrefetchScalarGridSpec(
        num_scalar_prefetch=lead, grid=grid, in_specs=in_specs, out_specs=out_specs
    )
    moved = sum(math.prod(a.shape) * a.dtype.itemsize for a in args[:inputs])
    return pl.pallas_call(
        body,
        grid_spec=spec,
        out_shape=out_shape,
        input_output_aliases=aliases,
        cost_estimate=pl.CostEstimate(
            flops=flops, bytes_accessed=moved, transcendentals=0
        ),
    )(*(() if prefetch is None else (prefetch,)), *args)


def whole(shape):
    return pl.BlockSpec(shape, lambda *_: (0,) * len(shape))


def row_sum(values):
    return jnp.sum(values, axis=0, keepdims=True)


def tally(step, sums, rows):
    @pl.when(step == 0)
    def _():
        sums[...] = jnp.zeros_like(sums)

    for index, row in enumerate(rows):
        sums[index : index + 1, :] += row


def rest_kernel(normed, own, first, second, third, is_odd, bias, triple, weight):
    @pl.when(pl.program_id(0) == 0)
    def _():
        for part in range(3):
            if part == 2:
                far = third[...]
            else:
                far = jnp.where(is_odd[0] == part, first[...], second[...])
            far = far.astype(LOW)
            weight[0, part] = own[part, :128]
            weight[1, part, :64] = own[part, 128:]
            weight[1, part, 64:] = far[:64]
            weight[2, part] = far[64:]

    rows = 2 * weight.shape[1] * weight.shape[2]
    rest = weight[1:].reshape(rows, weight.shape[3])
    triple[...] = (dot_last(normed[...], rest) + bias[...]).astype(LOW)


def grad_kernel(size, block, *refs):
    operands = refs[:size]
    is_odd, give, keep = refs[size:]
    full = jnp.concatenate(
        [
            dot_first(operands[i][...], operands[i + 1][...])
            for i in range(0, size, 2)
        ],
        axis=1,
    )
    odd = is_odd[0] == 1
    for index in range(give.shape[0]):
        at = 2 * index * block
        even_rows = full[at : at + block]
        odd_rows = full[at + block : at + 2 * block]
        give[index] = jnp.where(odd, even_rows, odd_rows)
        keep[index] = jnp.where(odd, odd_rows, even_rows)


def pack_kernel(first, second, third, fourth, out):
    rows = first.shape[0]
    for index, part in enumerate((first, second, third, fourth)):
        out[index * rows : (index + 1) * rows, :] = part[...].astype(LOW)


def front_kernel(tokens, vectors, weight, bias, normed, triple):
    unit, _ = normalize(tokens[...].astype(WIDE))
    low = (unit * vectors[0:1, :] + vectors[1:2, :]).astype(LOW)
    normed[...] = low
    rows = weight.shape[0] * weight.shape[1]
    triple[...] = (
        dot_last(low, weight[...].reshape(rows, weight.shape[2])) + bias[...]
    ).astype(LOW)


def low_head(block):
    lanes = lax.broadcasted_iota(jnp.int32, block.shape, 1)
    return lanes < block.shape[1] // 2


def head_of(block, head):
    wide = block.astype(WIDE)
    first = low_head(block)
    zero = jnp.zeros_like(wide)
    kept = jnp.where(first, wide, zero) if head == 0 else jnp.where(first, zero, wide)
    return kept.astype(LOW)


def parts_of(block):
    return block[:, :128], block[:, 128:256], block[:, 256:]


def same_image(ids):
    row = ids.astype(WIDE)
    return jnp.broadcast_to(row, (8, row.shape[1])).T[:, :1] == row


def attend_kernel(query_ids, triple, mixed, log_total):
    same = same_image(query_ids[0])
    query, keys, values = parts_of(triple[...])
    turned = values.astype(WIDE).T.astype(LOW)
    size = turned.shape[0] // 2
    parts = []
    for head in range(2):
        raw = dot_last(head_of(keys, head), query)
        raw = jnp.where(same, raw, NEGATIVE)
        top = jnp.max(raw, axis=0, keepdims=True)
        expo = jnp.exp2((raw - top) * (SCALE * LOG2E))
        total = jnp.sum(expo, axis=0, keepdims=True)
        probs = (expo * (1.0 / total)).astype(LOW)
        parts.append(dot(turned[head * size : (head + 1) * size], probs))
        log_total[0, 0, head : head + 1, :] = top * (SCALE * LOG2E) + jnp.log2(total)
    mixed[...] = jnp.concatenate(parts, axis=0).T.astype(LOW).astype(WIDE)


def attend(triple, query_ids, start, count):
    pairs = triple.shape[1] // 384
    return call(
        attend_kernel,
        (count, pairs),
        [
            pl.BlockSpec((1, 1, LEN), lambda s, p: (start + s, 0, 0)),
            pl.BlockSpec((LEN, 384), lambda s, p: (start + s, p)),
        ],
        [
            pl.BlockSpec((LEN, 128), lambda s, p: (s, p)),
            pl.BlockSpec((1, 1, 2, LEN), lambda s, p: (s, p, 0, 0)),
        ],
        [
            jax.ShapeDtypeStruct((count * LEN, pairs * 128), WIDE),
            jax.ShapeDtypeStruct((count, pairs, 2, LEN), WIDE),
        ],
        (query_ids, triple),
        flops=count * pairs * LEN * LEN * 1024,
    )


def attend_back_kernel(
    query_ids,
    triple_own,
    triple_rest,
    grad_mixed,
    log_own,
    log_rest,
    weight,
    own_pair,
    own_last,
    partial,
    sums,
):
    pair = pl.program_id(0)
    lead = pair == 0
    same = same_image(query_ids[0])
    block = jnp.where(
        lead, triple_own[...].astype(WIDE), triple_rest[...].astype(WIDE)
    ).astype(LOW)
    log_total = jnp.where(lead, log_own[0, 0], log_rest[0, 0])
    query, keys, values = parts_of(block)
    turned = keys.astype(WIDE).T.astype(LOW)
    size = turned.shape[0] // 2
    grad_query = []
    grad_keys = []
    grad_values = []
    for head in range(2):
        raw = dot_last(head_of(keys, head), query)
        scaled = jnp.where(same, raw * (SCALE * LOG2E), NEGATIVE)
        probs = jnp.exp2(scaled - log_total[head : head + 1, :])
        grad_probs = dot_last(head_of(values, head), grad_mixed[...])
        inner = jnp.sum(probs * grad_probs, axis=0, keepdims=True)
        grad_scores = (probs * (grad_probs - inner)).astype(LOW)
        grad_query.append(dot(turned[head * size : (head + 1) * size], grad_scores))
        grad_keys.append(dot(grad_scores, query))
        grad_values.append(dot(probs.astype(LOW), grad_mixed[...]))
    first = low_head(query)
    grads = jnp.concatenate(
        [
            SCALE * jnp.concatenate(grad_query, axis=0).T,
            SCALE * jnp.where(first, grad_keys[0], grad_keys[1]),
            jnp.where(first, grad_values[0], grad_values[1]),
        ],
        axis=1,
    ).astype(LOW)
    through = dot(grads, weight[...])
    tally(0, sums.at[0], [row_sum(grads.astype(WIDE))])

    @pl.when(lead)
    def _():
        own_pair[...] = grads
        partial[...] = through

    @pl.when(pair == 1)
    def _():
        own_last[...] = jnp.concatenate(
            [part[:, :64].astype(WIDE) for part in parts_of(grads)], axis=1
        ).astype(LOW)

    @pl.when(pair > 0)
    def _():
        partial[...] += through


def attend_back(
    triple_own, triple_rest, query_ids, grad_mixed, log_own, log_rest, weight, seq, shared
):
    rows = triple_own.shape[0]
    model = weight.shape[1]
    pairs = weight.shape[0] // 384

    def rest(p):
        return jnp.maximum(p - 1, 0)

    return call(
        attend_back_kernel,
        (pairs,),
        [
            pl.BlockSpec((1, 1, LEN), lambda p: (seq, 0, 0)),
            pl.BlockSpec((LEN, 384), lambda p: (seq, 0)),
            pl.BlockSpec((LEN, 384), lambda p: (seq, rest(p))),
            pl.BlockSpec((LEN, 128), lambda p: (0, p)),
            pl.BlockSpec((1, 1, 2, LEN), lambda p: (seq, 0, 0, 0)),
            pl.BlockSpec((1, 1, 2, LEN), lambda p: (0, rest(p), 0, 0)),
            pl.BlockSpec((384, model), lambda p: (p, 0)),
        ],
        [
            pl.BlockSpec((LEN, 384), lambda p: (seq, 0)),
            pl.BlockSpec((LEN, 192), lambda p: (seq, 0)),
            pl.BlockSpec((LEN, model), lambda p: (0, 0)),
            pl.BlockSpec((1, 8, 384), lambda p: (p, 0, 0)),
        ],
        [
            jax.ShapeDtypeStruct((rows, 384), LOW),
            jax.ShapeDtypeStruct((rows, 192), LOW),
            jax.ShapeDtypeStruct((LEN, model), WIDE),
            jax.ShapeDtypeStruct((pairs, 8, 384), WIDE),
        ],
        (query_ids, triple_own, triple_rest, grad_mixed, log_own, log_rest, weight),
        flops=pairs * LEN * LEN * 3328,
        shared=((0, shared[0]), (1, shared[1])),
    )


def gelu_parts(values):
    cdf = 0.5 * (1.0 + lax.erf(values * (0.5**0.5)))
    density = jnp.exp(-0.5 * values * values) * ((2.0 * math.pi) ** -0.5)
    return (values * cdf, cdf + values * density)


def middle_kernel(
    tokens,
    mixed_own,
    mixed_rest,
    other_own,
    other_rest,
    proj,
    vectors,
    up,
    up_bias,
    down,
    cotangent,
    middle,
    normed2,
    hidden,
    grad_pre,
    mixed_kept,
    back_give,
    back_keep,
    fed_give,
    fed_keep,
    sums,
):
    mixed = jnp.concatenate(
        [mixed_own[...], mixed_rest[...], other_own[...], other_rest[...]], axis=1
    ).astype(LOW)
    mixed_kept[...] = mixed[:, :192]
    summed = tokens[...].astype(WIDE) + dot(mixed, proj[...]) + vectors[2:3, :]
    middle[...] = summed
    unit, _ = normalize(summed)
    normed = (unit * vectors[3:4, :] + vectors[4:5, :]).astype(LOW)
    normed2[...] = normed
    activated, slope = gelu_parts(dot(normed, up[...]) + up_bias[...])
    kept = activated.astype(LOW)
    hidden[...] = kept
    grad = (dot_last(cotangent[...], down[...]) * slope).astype(LOW)
    grad_pre[...] = grad
    first = pl.program_id(0) == 0

    @pl.when(first)
    def _():
        back_give[...] = dot_last(grad, up[...])
        fed_give[...] = dot(kept, down[...])

    @pl.when(jnp.logical_not(first))
    def _():
        back_keep[...] = dot_last(grad, up[...])
        fed_keep[...] = dot(kept, down[...])

    tally(
        pl.program_id(0),
        sums,
        [row_sum(cotangent[...].astype(WIDE)), row_sum(grad.astype(WIDE))],
    )


def back_norm_kernel(
    total, other, is_odd, middle, cotangent, vectors, proj, grad_middle, low, grad_mixed, sums
):
    own = pl.program_id(0) == is_odd[0]
    normed_grad = jnp.where(own, total[...], other[...])
    unit, inverse = normalize(middle[...])
    piece = cotangent[...].astype(WIDE) + norm_backward(
        normed_grad, unit, inverse, vectors[3:4, :]
    )
    grad_middle[...] = piece
    rounded = piece.astype(LOW)
    low[...] = rounded
    grad_mixed[...] = dot_last(rounded, proj[...]).astype(LOW)
    tally(
        pl.program_id(0),
        sums,
        [row_sum(normed_grad * unit), row_sum(normed_grad), row_sum(piece)],
    )


def final_kernel(partial, other, tokens, grad_middle, vectors, input_grad, sums):
    normed_grad = partial[...] + other[...]
    unit, inverse = normalize(tokens[...].astype(WIDE))
    input_grad[...] = (
        grad_middle[...] + norm_backward(normed_grad, unit, inverse, vectors[0:1, :])
    ).astype(LOW)
    tally(pl.program_id(0), sums, [row_sum(normed_grad * unit), row_sum(normed_grad)])


def output_kernel(total, other, is_odd, middle, vectors, out):
    own = pl.program_id(0) == is_odd[0]
    fed = jnp.where(own, total[...], other[...])
    out[...] = (middle[...] + fed + vectors[5:6, :]).astype(LOW)


def shards(
    count_dp,
    tokens,
    segment_ids,
    first_gain,
    first_shift,
    qkv_weight,
    qv_bias,
    proj_weight,
    proj_bias,
    second_gain,
    second_shift,
    up_weight,
    up_bias,
    down_weight,
    down_bias,
    cotangent,
):
    rows, model = tokens.shape
    local = qv_bias.shape[1] * qv_bias.shape[2]
    hidden_size = up_weight.shape[1]
    count = rows // LEN
    odd = (lax.axis_index("mp") % 2).astype(jnp.int32).reshape(1)

    in_smem = pl.BlockSpec(memory_space=pltpu.SMEM)

    def row(values):
        return values.astype(WIDE).reshape(1, -1)

    def seq_half(width, seq):
        return pl.BlockSpec((HALF, width), lambda i: (2 * seq + i, 0))

    def half(width):
        return pl.BlockSpec((HALF, width), lambda i: (i, 0))

    own_rows = jnp.transpose(qkv_weight, (1, 2, 0))
    own_bias = qv_bias.reshape(2, local).astype(WIDE)
    far_bias = over_x(own_bias)
    dp_odd = (lax.axis_index("dp") % 2).astype(jnp.int32).reshape(1)
    far_first = over_x(jnp.where(dp_odd[0] == 1, own_rows[1], own_rows[0]).astype(WIDE))
    far_third = over_x(own_rows[2].astype(WIDE))
    far_second = over_dp(far_first, count_dp, 0)
    proj_wide = proj_weight.astype(WIDE)
    far_proj = over_x(proj_wide)
    core_proj = over_core(proj_wide)
    core_far_proj = over_core(far_proj)

    vectors = jnp.stack(
        [first_gain, first_shift, proj_bias, second_gain, second_shift, down_bias, down_bias, down_bias]
    ).astype(WIDE)
    vector_spec = whole((8, model))
    query_ids = segment_ids.reshape(count, 1, LEN)
    none = jnp.zeros((128,), WIDE)
    bias_own = row(jnp.concatenate([own_bias[0, :128], none, own_bias[1, :128]]))
    bias_rest = row(
        jnp.concatenate(
            [
                own_bias[0, 128:],
                far_bias[0, :64],
                none,
                own_bias[1, 128:],
                far_bias[1, :64],
                far_bias[0, 64:],
                none,
                far_bias[1, 64:],
            ]
        )
    )

    normed1, triple_own = call(
        front_kernel,
        (2 * count,),
        [
            half(model),
            vector_spec,
            whole((3, 128, model)),
            whole((1, 384)),
        ],
        [half(model), half(384)],
        [jax.ShapeDtypeStruct((rows, model), LOW), jax.ShapeDtypeStruct((rows, 384), LOW)],
        (tokens, vectors, own_rows, bias_own),
        flops=rows * model * 800,
    )
    mixed_own, log_own = attend(triple_own, query_ids, 0, count)
    other_own = over_core(mixed_own)

    triple_rest, weight_six = call(
        rest_kernel,
        (2 * count,),
        [
            half(model),
            whole((3, local, model)),
            whole((local, model)),
            whole((local, model)),
            whole((local, model)),
            in_smem,
            whole((1, 4 * local)),
        ],
        [half(4 * local), whole((3, 3, 128, model))],
        [
            jax.ShapeDtypeStruct((rows, 4 * local), LOW),
            jax.ShapeDtypeStruct((3, 3, 128, model), LOW),
        ],
        (normed1, own_rows, far_first, far_second, far_third, dp_odd, bias_rest),
        flops=rows * model * local * 8,
    )
    weight_six = weight_six.reshape(6 * local, model)
    proj_all = call(
        pack_kernel,
        (1,),
        [whole((local, model))] * 4,
        whole((4 * local, model)),
        jax.ShapeDtypeStruct((4 * local, model), LOW),
        (proj_weight, far_proj, core_proj, core_far_proj),
        flops=4 * local * model,
    )

    def picked(width, seq):
        return pl.BlockSpec(
            (HALF, width), lambda i, is_odd: (2 * seq + (i + 1 + is_odd[0]) % 2, 0)
        )

    attended = []
    for seq in range(count):
        mixed_rest, log_rest = attend(triple_rest, query_ids, seq, 1)
        attended.append((mixed_rest, log_rest, over_core(mixed_rest)))

    kept = [None] * 4
    middles = []
    mlp_sums = []
    back_chip = []
    fed_chip = []
    for seq in range(count):
        mixed_rest, _, other_rest = attended[seq]
        middle, *kept, back_give, back_keep, fed_give, fed_keep, sums = call(
            middle_kernel,
            (2,),
            [
                picked(model, seq),
                picked(128, seq),
                picked(256, 0),
                picked(128, seq),
                picked(256, 0),
                whole((model, model)),
                vector_spec,
                whole((model, hidden_size)),
                whole((1, hidden_size)),
                whole((hidden_size, model)),
                picked(model, seq),
            ],
            [
                picked(model, 0),
                picked(model, seq),
                picked(hidden_size, seq),
                picked(hidden_size, seq),
                picked(local, seq),
                *([whole((HALF, model))] * 4),
                whole((8, model)),
            ],
            [
                jax.ShapeDtypeStruct((LEN, model), WIDE),
                jax.ShapeDtypeStruct((rows, model), LOW),
                jax.ShapeDtypeStruct((rows, hidden_size), LOW),
                jax.ShapeDtypeStruct((rows, hidden_size), LOW),
                jax.ShapeDtypeStruct((rows, local), LOW),
                *([jax.ShapeDtypeStruct((HALF, model), WIDE)] * 4),
                jax.ShapeDtypeStruct((8, model), WIDE),
            ],
            (
                tokens,
                mixed_own,
                mixed_rest,
                other_own,
                other_rest,
                proj_all,
                vectors,
                up_weight,
                row(up_bias),
                down_weight,
                cotangent,
            ),
            flops=LEN * model * model * 10,
            prefetch=odd,
            shared=tuple((1 + i, kept[i]) for i in range(4)),
        )
        middles.append(middle)
        mlp_sums.append(sums)
        back_chip.append(back_keep + over_core(back_give))
        fed_chip.append(fed_keep + over_core(fed_give))
    normed2, hidden, grad_pre, mixed_kept = kept

    back_far = []
    for seq in range(count):
        back_far.append(over_x(back_chip[seq]))
    fed_far = []
    for seq in range(count):
        fed_far.append(over_x(fed_chip[seq]))

    def grad(*operands):
        width = sum(right.shape[1] for right in operands[1::2])
        block = model // count_dp
        part = pl.BlockSpec((count_dp // 4, block, width), lambda i: (i, 0, 0))
        return call(
            functools.partial(grad_kernel, len(operands), block),
            (2,),
            [
                whole(values.shape)
                if index % 2
                else pl.BlockSpec((rows, model // 2), lambda i: (0, i))
                for index, values in enumerate(operands)
            ]
            + [in_smem],
            [part, part],
            [jax.ShapeDtypeStruct((count_dp // 2, block, width), WIDE)] * 2,
            (*operands, dp_odd),
            flops=2 * rows * model * width,
        )

    down_part = scatter_dp(*grad(cotangent, hidden), count_dp)
    up_part = scatter_dp(*grad(normed2, grad_pre), count_dp)

    low_rows = None
    own_grads = [None, None]
    input_grad = None
    norm_sums = []
    attend_sums = []
    first_sums = []
    for seq in range(count):
        total = back_chip[seq] + back_far[seq]
        other = over_core(total)
        grad_middle, low_rows, grad_mixed, sums = call(
            back_norm_kernel,
            (2,),
            [
                whole((HALF, model)),
                whole((HALF, model)),
                in_smem,
                half(model),
                seq_half(model, seq),
                vector_spec,
                whole((2 * local, model)),
            ],
            [half(model), seq_half(model, seq), half(2 * local), whole((8, model))],
            [
                jax.ShapeDtypeStruct((LEN, model), WIDE),
                jax.ShapeDtypeStruct((rows, model), LOW),
                jax.ShapeDtypeStruct((LEN, 2 * local), LOW),
                jax.ShapeDtypeStruct((8, model), WIDE),
            ],
            (total, other, odd, middles[seq], cotangent, vectors, proj_all),
            flops=LEN * model * local * 8,
            shared=((1, low_rows),),
        )
        norm_sums.append(sums)
        *own_grads, partial, sums = attend_back(
            triple_own,
            triple_rest,
            query_ids,
            grad_mixed,
            log_own,
            attended[seq][1],
            weight_six,
            seq,
            own_grads,
        )
        attend_sums.append(sums)
        other = over_core(partial)
        input_grad, sums = call(
            final_kernel,
            (2,),
            [
                half(model),
                half(model),
                seq_half(model, seq),
                half(model),
                vector_spec,
            ],
            [seq_half(model, seq), whole((8, model))],
            [
                jax.ShapeDtypeStruct((rows, model), LOW),
                jax.ShapeDtypeStruct((8, model), WIDE),
            ],
            (partial, other, tokens, grad_middle, vectors),
            flops=LEN * model * 40,
            shared=((0, input_grad),),
        )
        first_sums.append(sums)

    pair_part = scatter_dp(*grad(normed1, own_grads[0]), count_dp)
    last_part = scatter_dp(*grad(normed1, own_grads[1], low_rows, mixed_kept), count_dp)
    proj_part = last_part[:, local:]
    last_part = last_part[:, :local]
    block = pair_part.shape[0]
    qkv_part = jnp.concatenate(
        [pair_part.reshape(block, 3, 128), last_part.reshape(block, 3, 64)], axis=2
    )

    layer_output = None
    for seq in range(count):
        total = fed_chip[seq] + fed_far[seq]
        other = over_core(total)
        layer_output = call(
            output_kernel,
            (2,),
            [
                whole((HALF, model)),
                whole((HALF, model)),
                in_smem,
                half(model),
                vector_spec,
            ],
            seq_half(model, seq),
            jax.ShapeDtypeStruct((rows, model), LOW),
            (total, other, odd, middles[seq], vectors),
            flops=LEN * model * 4,
            shared=((0, layer_output),),
        )

    mlp_sums = sum(mlp_sums)
    norm_sums = sum(norm_sums)
    attend_sums = sum(attend_sums)[:2, 0]
    first_sums = sum(first_sums)
    pair_sums = attend_sums[0].reshape(3, 128)
    last_sums = attend_sums[1].reshape(3, 128)[:, :64]
    qv_sums = jnp.concatenate([pair_sums, last_sums], axis=1)
    flat = jnp.concatenate(
        [
            first_sums[0],
            first_sums[1],
            norm_sums[2],
            norm_sums[0],
            norm_sums[1],
            mlp_sums[0],
            mlp_sums[1],
            qv_sums[0],
            qv_sums[2],
        ]
    )
    sums = sum_dp(flat, count_dp)
    here = lax.axis_index("dp")

    def share(values, axis):
        size = values.shape[axis] // count_dp
        return lax.dynamic_slice_in_dim(values, here * size, size, axis)

    vectors = share(sums[: 6 * model].reshape(6, model), 1)
    up_bias_sum = sums[6 * model : 6 * model + hidden_size].reshape(up_bias.shape)
    qv_sum = sums[6 * model + hidden_size :].reshape(qv_bias.shape)
    return (
        layer_output,
        input_grad,
        vectors[0],
        vectors[1],
        qkv_part,
        share(qv_sum, 2),
        proj_part.T,
        vectors[2],
        vectors[3],
        vectors[4],
        up_part,
        share(up_bias_sum, 1),
        down_part.T,
        vectors[5],
    )


def solution(mesh):
    count_dp = mesh.shape["dp"]

    def layer(*args):
        return shards(count_dp, *args)

    in_specs = (
        P("dp", None),
        P("dp"),
        P(),
        P(),
        P(None, None, "mp"),
        P(None, "mp", None),
        P("mp", None),
        P(),
        P(),
        P(),
        P(None, "mp"),
        P("mp", None),
        P("mp", None),
        P(),
        P("dp", None),
    )
    out_specs = (
        P("dp", None),
        P("dp", None),
        P("dp"),
        P("dp"),
        P("dp", None, "mp"),
        P(None, "mp", "dp"),
        P("mp", "dp"),
        P("dp"),
        P("dp"),
        P("dp"),
        P("dp", "mp"),
        P("mp", "dp"),
        P("mp", "dp"),
        P("dp"),
    )
    return jax.shard_map(layer, mesh=mesh, in_specs=in_specs, out_specs=out_specs, check_vma=False)
```

```python
import functools
import math

import jax
import jax.numpy as jnp
from jax import lax
from jax.experimental import pallas as pl
from jax.experimental.pallas import tpu as pltpu
from jax.sharding import PartitionSpec as P


LEN = 512
HALF = LEN // 2
EPS = 1e-06
SCALE = 0.125
NEGATIVE = -1e30
LOG2E = math.log2(math.e)
LOW = jnp.bfloat16
WIDE = jnp.float32


def normalize(values):
    centre = values - jnp.mean(values, axis=-1, keepdims=True)
    inverse = lax.rsqrt(jnp.mean(centre * centre, axis=-1, keepdims=True) + EPS)
    return (centre * inverse, inverse)


def norm_backward(grad_normed, unit, inverse, gain):
    scaled = grad_normed * gain
    return inverse * (
        scaled
        - jnp.mean(scaled, axis=-1, keepdims=True)
        - unit * jnp.mean(scaled * unit, axis=-1, keepdims=True)
    )


def over_x(values):
    return lax.ppermute(values, "mp", [(i, i ^ 2) for i in range(4)])


def over_core(values):
    return lax.ppermute(values, "mp", [(i, i ^ 1) for i in range(4)])


def over_dp(values, count, bit):
    return lax.ppermute(values, "dp", [(i, i ^ (1 << bit)) for i in range(count)])


def scatter_dp(give, keep, count):
    here = lax.axis_index("dp")
    _, block, width = keep.shape
    got = over_dp(give, count, 0)
    held = keep + got
    before = held
    for bit in range(1, count.bit_length() - 1):
        before = held
        mine = (here >> bit) & 1
        split = held.reshape(held.shape[0] // 2, 2, block, width)
        keep = lax.dynamic_index_in_dim(split, mine, 1, keepdims=False)
        give = lax.dynamic_index_in_dim(split, 1 - mine, 1, keepdims=False)
        got = over_dp(give, count, bit)
        held = keep + got
    return held[0], before


def sum_dp(values, count):
    for bit in range(count.bit_length() - 1):
        got = over_dp(values, count, bit)
        values = values + got
    return values


def dot_last(left, right):
    return lax.dot_general(
        left, right, (((1,), (1,)), ((), ())), preferred_element_type=WIDE
    )


def dot_first(left, right):
    return lax.dot_general(
        left, right, (((0,), (0,)), ((), ())), preferred_element_type=WIDE
    )


def dot(left, right):
    return jnp.dot(left, right, preferred_element_type=WIDE)


def call(kernel, grid, in_specs, out_specs, out_shape, args, flops, prefetch=None, shared=()):
    args = list(args)
    in_specs = list(in_specs)
    aliases = {}
    lead = 0 if prefetch is None else 1
    inputs = len(args)
    for index, buffer in shared:
        if buffer is not None:
            aliases[lead + len(args)] = index
            args.append(buffer)
            in_specs.append(pl.BlockSpec(memory_space=pl.ANY))
    extra = len(args) - inputs

    def body(*refs):
        refs = refs[lead:]
        kernel(*refs[:inputs], *refs[inputs + extra :])

    spec = pltpu.PrefetchScalarGridSpec(
        num_scalar_prefetch=lead, grid=grid, in_specs=in_specs, out_specs=out_specs
    )
    moved = sum(math.prod(a.shape) * a.dtype.itemsize for a in args[:inputs])
    return pl.pallas_call(
        body,
        grid_spec=spec,
        out_shape=out_shape,
        input_output_aliases=aliases,
        cost_estimate=pl.CostEstimate(
            flops=flops, bytes_accessed=moved, transcendentals=0
        ),
    )(*(() if prefetch is None else (prefetch,)), *args)


def whole(shape):
    return pl.BlockSpec(shape, lambda *_: (0,) * len(shape))


def row_sum(values):
    return jnp.sum(values, axis=0, keepdims=True)


def tally(step, sums, rows):
    @pl.when(step == 0)
    def _():
        sums[...] = jnp.zeros_like(sums)

    for index, row in enumerate(rows):
        sums[index : index + 1, :] += row


def rest_kernel(normed, own, first, second, third, is_odd, bias, triple, weight):
    @pl.when(pl.program_id(0) == 0)
    def _():
        for part in range(3):
            if part == 2:
                far = third[...]
            else:
                far = jnp.where(is_odd[0] == part, first[...], second[...])
            far = far.astype(LOW)
            weight[0, part] = own[part, :128]
            weight[1, part, :64] = own[part, 128:]
            weight[1, part, 64:] = far[:64]
            weight[2, part] = far[64:]

    rows = 2 * weight.shape[1] * weight.shape[2]
    rest = weight[1:].reshape(rows, weight.shape[3])
    triple[...] = (dot_last(normed[...], rest) + bias[...]).astype(LOW)


def grad_kernel(block, left, right, is_odd, give, keep):
    full = dot_first(left[...], right[...])
    odd = is_odd[0] == 1
    for index in range(give.shape[0]):
        at = 2 * index * block
        even_rows = full[at : at + block]
        odd_rows = full[at + block : at + 2 * block]
        give[index] = jnp.where(odd, even_rows, odd_rows)
        keep[index] = jnp.where(odd, odd_rows, even_rows)


def pack_kernel(first, second, third, fourth, out):
    rows = first.shape[0]
    for index, part in enumerate((first, second, third, fourth)):
        out[index * rows : (index + 1) * rows, :] = part[...].astype(LOW)


def front_kernel(tokens, vectors, weight, bias, normed, triple):
    unit, _ = normalize(tokens[...].astype(WIDE))
    low = (unit * vectors[0:1, :] + vectors[1:2, :]).astype(LOW)
    normed[...] = low
    rows = weight.shape[0] * weight.shape[1]
    triple[...] = (
        dot_last(low, weight[...].reshape(rows, weight.shape[2])) + bias[...]
    ).astype(LOW)


def low_head(block):
    lanes = lax.broadcasted_iota(jnp.int32, block.shape, 1)
    return lanes < block.shape[1] // 2


def head_of(block, head):
    wide = block.astype(WIDE)
    first = low_head(block)
    zero = jnp.zeros_like(wide)
    kept = jnp.where(first, wide, zero) if head == 0 else jnp.where(first, zero, wide)
    return kept.astype(LOW)


def parts_of(block):
    return block[:, :128], block[:, 128:256], block[:, 256:]


def same_image(ids):
    row = ids.astype(WIDE)
    return jnp.broadcast_to(row, (8, row.shape[1])).T[:, :1] == row


def attend_kernel(query_ids, triple, mixed, log_total):
    same = same_image(query_ids[0])
    query, keys, values = parts_of(triple[...])
    turned = values.astype(WIDE).T.astype(LOW)
    size = turned.shape[0] // 2
    parts = []
    for head in range(2):
        raw = dot_last(head_of(keys, head), query)
        raw = jnp.where(same, raw, NEGATIVE)
        top = jnp.max(raw, axis=0, keepdims=True)
        expo = jnp.exp2((raw - top) * (SCALE * LOG2E))
        total = jnp.sum(expo, axis=0, keepdims=True)
        probs = (expo * (1.0 / total)).astype(LOW)
        parts.append(dot(turned[head * size : (head + 1) * size], probs))
        log_total[0, 0, head : head + 1, :] = top * (SCALE * LOG2E) + jnp.log2(total)
    mixed[...] = jnp.concatenate(parts, axis=0).T.astype(LOW).astype(WIDE)


def attend(triple, query_ids, start, count):
    pairs = triple.shape[1] // 384
    return call(
        attend_kernel,
        (count, pairs),
        [
            pl.BlockSpec((1, 1, LEN), lambda s, p: (start + s, 0, 0)),
            pl.BlockSpec((LEN, 384), lambda s, p: (start + s, p)),
        ],
        [
            pl.BlockSpec((LEN, 128), lambda s, p: (s, p)),
            pl.BlockSpec((1, 1, 2, LEN), lambda s, p: (s, p, 0, 0)),
        ],
        [
            jax.ShapeDtypeStruct((count * LEN, pairs * 128), WIDE),
            jax.ShapeDtypeStruct((count, pairs, 2, LEN), WIDE),
        ],
        (query_ids, triple),
        flops=count * pairs * LEN * LEN * 1024,
    )


def attend_back_kernel(
    query_ids,
    triple_own,
    triple_rest,
    grad_mixed,
    log_own,
    log_rest,
    weight,
    own_pair,
    own_last,
    partial,
    sums,
):
    pair = pl.program_id(0)
    lead = pair == 0
    same = same_image(query_ids[0])
    block = jnp.where(
        lead, triple_own[...].astype(WIDE), triple_rest[...].astype(WIDE)
    ).astype(LOW)
    log_total = jnp.where(lead, log_own[0, 0], log_rest[0, 0])
    query, keys, values = parts_of(block)
    turned = keys.astype(WIDE).T.astype(LOW)
    size = turned.shape[0] // 2
    grad_query = []
    grad_keys = []
    grad_values = []
    for head in range(2):
        raw = dot_last(head_of(keys, head), query)
        scaled = jnp.where(same, raw * (SCALE * LOG2E), NEGATIVE)
        probs = jnp.exp2(scaled - log_total[head : head + 1, :])
        grad_probs = dot_last(head_of(values, head), grad_mixed[...])
        inner = jnp.sum(probs * grad_probs, axis=0, keepdims=True)
        grad_scores = (probs * (grad_probs - inner)).astype(LOW)
        grad_query.append(dot(turned[head * size : (head + 1) * size], grad_scores))
        grad_keys.append(dot(grad_scores, query))
        grad_values.append(dot(probs.astype(LOW), grad_mixed[...]))
    first = low_head(query)
    grads = jnp.concatenate(
        [
            SCALE * jnp.concatenate(grad_query, axis=0).T,
            SCALE * jnp.where(first, grad_keys[0], grad_keys[1]),
            jnp.where(first, grad_values[0], grad_values[1]),
        ],
        axis=1,
    ).astype(LOW)
    through = dot(grads, weight[...])
    tally(0, sums.at[0], [row_sum(grads.astype(WIDE))])

    @pl.when(lead)
    def _():
        own_pair[...] = grads
        partial[...] = through

    @pl.when(pair == 1)
    def _():
        own_last[...] = jnp.concatenate(
            [part[:, :64].astype(WIDE) for part in parts_of(grads)], axis=1
        ).astype(LOW)

    @pl.when(pair > 0)
    def _():
        partial[...] += through


def attend_back(
    triple_own, triple_rest, query_ids, grad_mixed, log_own, log_rest, weight, seq, shared
):
    rows = triple_own.shape[0]
    model = weight.shape[1]
    pairs = weight.shape[0] // 384

    def rest(p):
        return jnp.maximum(p - 1, 0)

    return call(
        attend_back_kernel,
        (pairs,),
        [
            pl.BlockSpec((1, 1, LEN), lambda p: (seq, 0, 0)),
            pl.BlockSpec((LEN, 384), lambda p: (seq, 0)),
            pl.BlockSpec((LEN, 384), lambda p: (seq, rest(p))),
            pl.BlockSpec((LEN, 128), lambda p: (0, p)),
            pl.BlockSpec((1, 1, 2, LEN), lambda p: (seq, 0, 0, 0)),
            pl.BlockSpec((1, 1, 2, LEN), lambda p: (0, rest(p), 0, 0)),
            pl.BlockSpec((384, model), lambda p: (p, 0)),
        ],
        [
            pl.BlockSpec((LEN, 384), lambda p: (seq, 0)),
            pl.BlockSpec((LEN, 192), lambda p: (seq, 0)),
            pl.BlockSpec((LEN, model), lambda p: (0, 0)),
            pl.BlockSpec((1, 8, 384), lambda p: (p, 0, 0)),
        ],
        [
            jax.ShapeDtypeStruct((rows, 384), LOW),
            jax.ShapeDtypeStruct((rows, 192), LOW),
            jax.ShapeDtypeStruct((LEN, model), WIDE),
            jax.ShapeDtypeStruct((pairs, 8, 384), WIDE),
        ],
        (query_ids, triple_own, triple_rest, grad_mixed, log_own, log_rest, weight),
        flops=pairs * LEN * LEN * 3328,
        shared=((0, shared[0]), (1, shared[1])),
    )


def gelu_parts(values):
    cdf = 0.5 * (1.0 + lax.erf(values * (0.5**0.5)))
    density = jnp.exp(-0.5 * values * values) * ((2.0 * math.pi) ** -0.5)
    return (values * cdf, cdf + values * density)


def middle_kernel(
    tokens,
    mixed_own,
    mixed_rest,
    other_own,
    other_rest,
    proj,
    vectors,
    up,
    up_bias,
    down,
    cotangent,
    middle,
    normed2,
    hidden,
    grad_pre,
    mixed_kept,
    back_give,
    back_keep,
    fed_give,
    fed_keep,
    sums,
):
    mixed = jnp.concatenate(
        [mixed_own[...], mixed_rest[...], other_own[...], other_rest[...]], axis=1
    ).astype(LOW)
    mixed_kept[...] = mixed[:, :192]
    summed = tokens[...].astype(WIDE) + dot(mixed, proj[...]) + vectors[2:3, :]
    middle[...] = summed
    unit, _ = normalize(summed)
    normed = (unit * vectors[3:4, :] + vectors[4:5, :]).astype(LOW)
    normed2[...] = normed
    activated, slope = gelu_parts(dot(normed, up[...]) + up_bias[...])
    kept = activated.astype(LOW)
    hidden[...] = kept
    grad = (dot_last(cotangent[...], down[...]) * slope).astype(LOW)
    grad_pre[...] = grad
    back_keep[...] = dot_last(grad, up[...])
    fed_keep[...] = dot(kept, down[...])

    @pl.when(pl.program_id(0) == 0)
    def _():
        back_give[...] = back_keep[...]
        fed_give[...] = fed_keep[...]

    tally(
        pl.program_id(0),
        sums,
        [row_sum(cotangent[...].astype(WIDE)), row_sum(grad.astype(WIDE))],
    )


def back_norm_kernel(
    total, other, is_odd, middle, cotangent, vectors, proj, grad_middle, low, grad_mixed, sums
):
    own = pl.program_id(0) == is_odd[0]
    normed_grad = jnp.where(own, total[...], other[...])
    unit, inverse = normalize(middle[...])
    piece = cotangent[...].astype(WIDE) + norm_backward(
        normed_grad, unit, inverse, vectors[3:4, :]
    )
    grad_middle[...] = piece
    rounded = piece.astype(LOW)
    low[...] = rounded
    grad_mixed[...] = dot_last(rounded, proj[...]).astype(LOW)
    tally(
        pl.program_id(0),
        sums,
        [row_sum(normed_grad * unit), row_sum(normed_grad), row_sum(piece)],
    )


def final_kernel(partial, other, tokens, grad_middle, vectors, input_grad, sums):
    normed_grad = partial[...] + other[...]
    unit, inverse = normalize(tokens[...].astype(WIDE))
    input_grad[...] = (
        grad_middle[...] + norm_backward(normed_grad, unit, inverse, vectors[0:1, :])
    ).astype(LOW)
    tally(pl.program_id(0), sums, [row_sum(normed_grad * unit), row_sum(normed_grad)])


def output_kernel(total, other, is_odd, middle, vectors, out):
    own = pl.program_id(0) == is_odd[0]
    fed = jnp.where(own, total[...], other[...])
    out[...] = (middle[...] + fed + vectors[5:6, :]).astype(LOW)


def shards(
    count_dp,
    tokens,
    segment_ids,
    first_gain,
    first_shift,
    qkv_weight,
    qv_bias,
    proj_weight,
    proj_bias,
    second_gain,
    second_shift,
    up_weight,
    up_bias,
    down_weight,
    down_bias,
    cotangent,
):
    rows, model = tokens.shape
    local = qv_bias.shape[1] * qv_bias.shape[2]
    hidden_size = up_weight.shape[1]
    count = rows // LEN
    odd = (lax.axis_index("mp") % 2).astype(jnp.int32).reshape(1)

    in_smem = pl.BlockSpec(memory_space=pltpu.SMEM)

    def row(values):
        return values.astype(WIDE).reshape(1, -1)

    def seq_half(width, seq):
        return pl.BlockSpec((HALF, width), lambda i: (2 * seq + i, 0))

    def half(width):
        return pl.BlockSpec((HALF, width), lambda i: (i, 0))

    own_rows = jnp.transpose(qkv_weight, (1, 2, 0))
    own_bias = qv_bias.reshape(2, local).astype(WIDE)
    far_bias = over_x(own_bias)
    dp_odd = (lax.axis_index("dp") % 2).astype(jnp.int32).reshape(1)
    far_first = over_x(jnp.where(dp_odd[0] == 1, own_rows[1], own_rows[0]).astype(WIDE))
    far_third = over_x(own_rows[2].astype(WIDE))
    far_second = over_dp(far_first, count_dp, 0)
    proj_wide = proj_weight.astype(WIDE)
    far_proj = over_x(proj_wide)
    core_proj = over_core(proj_wide)
    core_far_proj = over_core(far_proj)

    vectors = jnp.stack(
        [first_gain, first_shift, proj_bias, second_gain, second_shift, down_bias, down_bias, down_bias]
    ).astype(WIDE)
    vector_spec = whole((8, model))
    query_ids = segment_ids.reshape(count, 1, LEN)
    none = jnp.zeros((128,), WIDE)
    bias_own = row(jnp.concatenate([own_bias[0, :128], none, own_bias[1, :128]]))
    bias_rest = row(
        jnp.concatenate(
            [
                own_bias[0, 128:],
                far_bias[0, :64],
                none,
                own_bias[1, 128:],
                far_bias[1, :64],
                far_bias[0, 64:],
                none,
                far_bias[1, 64:],
            ]
        )
    )

    normed1, triple_own = call(
        front_kernel,
        (2 * count,),
        [
            half(model),
            vector_spec,
            whole((3, 128, model)),
            whole((1, 384)),
        ],
        [half(model), half(384)],
        [jax.ShapeDtypeStruct((rows, model), LOW), jax.ShapeDtypeStruct((rows, 384), LOW)],
        (tokens, vectors, own_rows, bias_own),
        flops=rows * model * 800,
    )
    mixed_own, log_own = attend(triple_own, query_ids, 0, count)
    other_own = over_core(mixed_own)

    triple_rest, weight_six = call(
        rest_kernel,
        (2 * count,),
        [
            half(model),
            whole((3, local, model)),
            whole((local, model)),
            whole((local, model)),
            whole((local, model)),
            in_smem,
            whole((1, 4 * local)),
        ],
        [half(4 * local), whole((3, 3, 128, model))],
        [
            jax.ShapeDtypeStruct((rows, 4 * local), LOW),
            jax.ShapeDtypeStruct((3, 3, 128, model), LOW),
        ],
        (normed1, own_rows, far_first, far_second, far_third, dp_odd, bias_rest),
        flops=rows * model * local * 8,
    )
    weight_six = weight_six.reshape(6 * local, model)
    proj_all = call(
        pack_kernel,
        (1,),
        [whole((local, model))] * 4,
        whole((4 * local, model)),
        jax.ShapeDtypeStruct((4 * local, model), LOW),
        (proj_weight, far_proj, core_proj, core_far_proj),
        flops=4 * local * model,
    )

    def picked(width, seq):
        return pl.BlockSpec(
            (HALF, width), lambda i, is_odd: (2 * seq + (i + 1 + is_odd[0]) % 2, 0)
        )

    attended = []
    for seq in range(count):
        mixed_rest, log_rest = attend(triple_rest, query_ids, seq, 1)
        attended.append((mixed_rest, log_rest, over_core(mixed_rest)))

    kept = [None] * 4
    middles = []
    mlp_sums = []
    back_chip = []
    fed_chip = []
    for seq in range(count):
        mixed_rest, _, other_rest = attended[seq]
        middle, *kept, back_give, back_keep, fed_give, fed_keep, sums = call(
            middle_kernel,
            (2,),
            [
                picked(model, seq),
                picked(128, seq),
                picked(256, 0),
                picked(128, seq),
                picked(256, 0),
                whole((model, model)),
                vector_spec,
                whole((model, hidden_size)),
                whole((1, hidden_size)),
                whole((hidden_size, model)),
                picked(model, seq),
            ],
            [
                picked(model, 0),
                picked(model, seq),
                picked(hidden_size, seq),
                picked(hidden_size, seq),
                picked(local, seq),
                *([whole((HALF, model))] * 4),
                whole((8, model)),
            ],
            [
                jax.ShapeDtypeStruct((LEN, model), WIDE),
                jax.ShapeDtypeStruct((rows, model), LOW),
                jax.ShapeDtypeStruct((rows, hidden_size), LOW),
                jax.ShapeDtypeStruct((rows, hidden_size), LOW),
                jax.ShapeDtypeStruct((rows, local), LOW),
                *([jax.ShapeDtypeStruct((HALF, model), WIDE)] * 4),
                jax.ShapeDtypeStruct((8, model), WIDE),
            ],
            (
                tokens,
                mixed_own,
                mixed_rest,
                other_own,
                other_rest,
                proj_all,
                vectors,
                up_weight,
                row(up_bias),
                down_weight,
                cotangent,
            ),
            flops=LEN * model * model * 10,
            prefetch=odd,
            shared=tuple((1 + i, kept[i]) for i in range(4)),
        )
        middles.append(middle)
        mlp_sums.append(sums)
        back_chip.append(back_keep + over_core(back_give))
        fed_chip.append(fed_keep + over_core(fed_give))
    normed2, hidden, grad_pre, mixed_kept = kept

    back_far = []
    for seq in range(count):
        back_far.append(over_x(back_chip[seq]))
    fed_far = []
    for seq in range(count):
        fed_far.append(over_x(fed_chip[seq]))

    def grad(*operands):
        width = operands[1].shape[1]
        tile = min(width, 384)
        block = model // count_dp
        part = pl.BlockSpec((count_dp // 4, block, tile), lambda i, j: (i, 0, j))
        return call(
            functools.partial(grad_kernel, block),
            (2, width // tile),
            [
                pl.BlockSpec((rows, model // 2), lambda i, j: (0, i)),
                pl.BlockSpec((rows, tile), lambda i, j: (0, j)),
                in_smem,
            ],
            [part, part],
            [jax.ShapeDtypeStruct((count_dp // 2, block, width), WIDE)] * 2,
            (*operands, dp_odd),
            flops=2 * rows * model * width,
        )

    down_part, _ = scatter_dp(*grad(cotangent, hidden), count_dp)
    up_part, _ = scatter_dp(*grad(normed2, grad_pre), count_dp)

    low_rows = None
    own_grads = [None, None]
    input_grad = None
    norm_sums = []
    attend_sums = []
    first_sums = []
    for seq in range(count):
        total = back_chip[seq] + back_far[seq]
        other = over_core(total)
        grad_middle, low_rows, grad_mixed, sums = call(
            back_norm_kernel,
            (2,),
            [
                whole((HALF, model)),
                whole((HALF, model)),
                in_smem,
                half(model),
                seq_half(model, seq),
                vector_spec,
                whole((2 * local, model)),
            ],
            [half(model), seq_half(model, seq), half(2 * local), whole((8, model))],
            [
                jax.ShapeDtypeStruct((LEN, model), WIDE),
                jax.ShapeDtypeStruct((rows, model), LOW),
                jax.ShapeDtypeStruct((LEN, 2 * local), LOW),
                jax.ShapeDtypeStruct((8, model), WIDE),
            ],
            (total, other, odd, middles[seq], cotangent, vectors, proj_all),
            flops=LEN * model * local * 8,
            shared=((1, low_rows),),
        )
        norm_sums.append(sums)
        *own_grads, partial, sums = attend_back(
            triple_own,
            triple_rest,
            query_ids,
            grad_mixed,
            log_own,
            attended[seq][1],
            weight_six,
            seq,
            own_grads,
        )
        attend_sums.append(sums)
        other = over_core(partial)

        def part(width):
            return pl.BlockSpec((HALF // 2, width), lambda i: (i, 0))

        def seq_part(width, seq=seq):
            return pl.BlockSpec((HALF // 2, width), lambda i: (4 * seq + i, 0))

        input_grad, sums = call(
            final_kernel,
            (4,),
            [
                part(model),
                part(model),
                seq_part(model),
                part(model),
                vector_spec,
            ],
            [seq_part(model), whole((8, model))],
            [
                jax.ShapeDtypeStruct((rows, model), LOW),
                jax.ShapeDtypeStruct((8, model), WIDE),
            ],
            (partial, other, tokens, grad_middle, vectors),
            flops=LEN * model * 40,
            shared=((0, input_grad),),
        )
        first_sums.append(sums)

    proj_part, early = scatter_dp(*grad(low_rows, mixed_kept), count_dp)
    pair_part, _ = scatter_dp(*grad(normed1, own_grads[0]), count_dp)
    own_last, _ = lax.optimization_barrier((own_grads[1], early))
    last_part, _ = scatter_dp(*grad(normed1, own_last), count_dp)
    block = pair_part.shape[0]
    qkv_part = jnp.concatenate(
        [pair_part.reshape(block, 3, 128), last_part.reshape(block, 3, 64)], axis=2
    )

    layer_output = None
    for seq in range(count):
        total = fed_chip[seq] + fed_far[seq]
        other = over_core(total)
        layer_output = call(
            output_kernel,
            (2,),
            [
                whole((HALF, model)),
                whole((HALF, model)),
                in_smem,
                half(model),
                vector_spec,
            ],
            seq_half(model, seq),
            jax.ShapeDtypeStruct((rows, model), LOW),
            (total, other, odd, middles[seq], vectors),
            flops=LEN * model * 4,
            shared=((0, layer_output),),
        )

    mlp_sums = sum(mlp_sums)
    norm_sums = sum(norm_sums)
    attend_sums = sum(attend_sums)[:2, 0]
    first_sums = sum(first_sums)
    pair_sums = attend_sums[0].reshape(3, 128)
    last_sums = attend_sums[1].reshape(3, 128)[:, :64]
    qv_sums = jnp.concatenate([pair_sums, last_sums], axis=1)
    flat = jnp.concatenate(
        [
            first_sums[0],
            first_sums[1],
            norm_sums[2],
            norm_sums[0],
            norm_sums[1],
            mlp_sums[0],
            mlp_sums[1],
            qv_sums[0],
            qv_sums[2],
        ]
    )
    sums = sum_dp(flat, count_dp)
    here = lax.axis_index("dp")

    def share(values, axis):
        size = values.shape[axis] // count_dp
        return lax.dynamic_slice_in_dim(values, here * size, size, axis)

    vectors = share(sums[: 6 * model].reshape(6, model), 1)
    up_bias_sum = sums[6 * model : 6 * model + hidden_size].reshape(up_bias.shape)
    qv_sum = sums[6 * model + hidden_size :].reshape(qv_bias.shape)
    return (
        layer_output,
        input_grad,
        vectors[0],
        vectors[1],
        qkv_part,
        share(qv_sum, 2),
        proj_part.T,
        vectors[2],
        vectors[3],
        vectors[4],
        up_part,
        share(up_bias_sum, 1),
        down_part.T,
        vectors[5],
    )


def solution(mesh):
    count_dp = mesh.shape["dp"]

    def layer(*args):
        return shards(count_dp, *args)

    in_specs = (
        P("dp", None),
        P("dp"),
        P(),
        P(),
        P(None, None, "mp"),
        P(None, "mp", None),
        P("mp", None),
        P(),
        P(),
        P(),
        P(None, "mp"),
        P("mp", None),
        P("mp", None),
        P(),
        P("dp", None),
    )
    out_specs = (
        P("dp", None),
        P("dp", None),
        P("dp"),
        P("dp"),
        P("dp", None, "mp"),
        P(None, "mp", "dp"),
        P("mp", "dp"),
        P("dp"),
        P("dp"),
        P("dp"),
        P("dp", "mp"),
        P("mp", "dp"),
        P("mp", "dp"),
        P("dp"),
    )
    return jax.shard_map(layer, mesh=mesh, in_specs=in_specs, out_specs=out_specs, check_vma=False)
```

```python
import functools
import math

import jax
import jax.numpy as jnp
from jax import lax
from jax.experimental import pallas as pl
from jax.experimental.pallas import tpu as pltpu
from jax.sharding import PartitionSpec as P


LEN = 512
HALF = LEN // 2
TILE = 768
EPS = 1e-06
SCALE = 0.125
NEGATIVE = -1e30
LOG2E = math.log2(math.e)
LOW = jnp.bfloat16
WIDE = jnp.float32


def normalize(values):
    centre = values - jnp.mean(values, axis=-1, keepdims=True)
    inverse = lax.rsqrt(jnp.mean(centre * centre, axis=-1, keepdims=True) + EPS)
    return (centre * inverse, inverse)


def norm_backward(grad_normed, unit, inverse, gain):
    scaled = grad_normed * gain
    return inverse * (
        scaled
        - jnp.mean(scaled, axis=-1, keepdims=True)
        - unit * jnp.mean(scaled * unit, axis=-1, keepdims=True)
    )


def over_x(values):
    return lax.ppermute(values, "mp", [(i, i ^ 2) for i in range(4)])


def over_core(values):
    return lax.ppermute(values, "mp", [(i, i ^ 1) for i in range(4)])


def over_dp(values, count, bit):
    return lax.ppermute(values, "dp", [(i, i ^ (1 << bit)) for i in range(count)])


def scatter_dp(give, keep, count):
    here = lax.axis_index("dp")
    _, block, width = keep.shape
    got = over_dp(give, count, 0)
    held = keep + got
    for bit in range(1, count.bit_length() - 1):
        mine = (here >> bit) & 1
        split = held.reshape(held.shape[0] // 2, 2, block, width)
        keep = lax.dynamic_index_in_dim(split, mine, 1, keepdims=False)
        give = lax.dynamic_index_in_dim(split, 1 - mine, 1, keepdims=False)
        got = over_dp(give, count, bit)
        held = keep + got
    return held[0]


def sum_dp(values, count):
    for bit in range(count.bit_length() - 1):
        got = over_dp(values, count, bit)
        values = values + got
    return values


def dot_last(left, right):
    return lax.dot_general(
        left, right, (((1,), (1,)), ((), ())), preferred_element_type=WIDE
    )


def dot_first(left, right):
    return lax.dot_general(
        left, right, (((0,), (0,)), ((), ())), preferred_element_type=WIDE
    )


def dot(left, right):
    return jnp.dot(left, right, preferred_element_type=WIDE)


def call(kernel, grid, in_specs, out_specs, out_shape, args, flops, prefetch=None, shared=()):
    args = list(args)
    in_specs = list(in_specs)
    aliases = {}
    lead = 0 if prefetch is None else 1
    inputs = len(args)
    for index, buffer in shared:
        if buffer is not None:
            aliases[lead + len(args)] = index
            args.append(buffer)
            in_specs.append(pl.BlockSpec(memory_space=pl.ANY))
    extra = len(args) - inputs

    def body(*refs):
        refs = refs[lead:]
        kernel(*refs[:inputs], *refs[inputs + extra :])

    spec = pltpu.PrefetchScalarGridSpec(
        num_scalar_prefetch=lead, grid=grid, in_specs=in_specs, out_specs=out_specs
    )
    moved = sum(math.prod(a.shape) * a.dtype.itemsize for a in args[:inputs])
    return pl.pallas_call(
        body,
        grid_spec=spec,
        out_shape=out_shape,
        input_output_aliases=aliases,
        cost_estimate=pl.CostEstimate(
            flops=flops, bytes_accessed=moved, transcendentals=0
        ),
    )(*(() if prefetch is None else (prefetch,)), *args)


def whole(shape):
    return pl.BlockSpec(shape, lambda *_: (0,) * len(shape))


def row_sum(values):
    return jnp.sum(values, axis=0, keepdims=True)


def tally(step, sums, rows):
    @pl.when(step == 0)
    def _():
        sums[...] = jnp.zeros_like(sums)

    for index, row in enumerate(rows):
        sums[index : index + 1, :] += row


def rest_kernel(normed, own, first, second, third, is_odd, bias, triple, weight):
    @pl.when(pl.program_id(0) == 0)
    def _():
        for part in range(3):
            if part == 2:
                far = third[...]
            else:
                far = jnp.where(is_odd[0] == part, first[...], second[...])
            far = far.astype(LOW)
            weight[0, part] = own[part, :128]
            weight[1, part, :64] = own[part, 128:]
            weight[1, part, 64:] = far[:64]
            weight[2, part] = far[64:]

    rows = 2 * weight.shape[1] * weight.shape[2]
    rest = weight[1:].reshape(rows, weight.shape[3])
    triple[...] = (dot_last(normed[...], rest) + bias[...]).astype(LOW)


def grad_kernel(block, *refs):
    *operands, is_odd, give, keep = refs
    full = jnp.concatenate(
        [
            dot_first(operands[i][...], operands[i + 1][...])
            for i in range(0, len(operands), 2)
        ],
        axis=1,
    )
    odd = is_odd[0] == 1
    for index in range(give.shape[0]):
        at = 2 * index * block
        even_rows = full[at : at + block]
        odd_rows = full[at + block : at + 2 * block]
        give[index] = jnp.where(odd, even_rows, odd_rows)
        keep[index] = jnp.where(odd, odd_rows, even_rows)


def pack_kernel(first, second, third, fourth, out):
    rows = first.shape[0]
    for index, part in enumerate((first, second, third, fourth)):
        out[index * rows : (index + 1) * rows, :] = part[...].astype(LOW)


def front_kernel(tokens, vectors, weight, bias, normed, triple):
    unit, _ = normalize(tokens[...].astype(WIDE))
    low = (unit * vectors[0:1, :] + vectors[1:2, :]).astype(LOW)
    normed[...] = low
    rows = weight.shape[0] * weight.shape[1]
    triple[...] = (
        dot_last(low, weight[...].reshape(rows, weight.shape[2])) + bias[...]
    ).astype(LOW)


def low_head(block):
    lanes = lax.broadcasted_iota(jnp.int32, block.shape, 1)
    return lanes < block.shape[1] // 2


def head_of(block, head):
    wide = block.astype(WIDE)
    first = low_head(block)
    zero = jnp.zeros_like(wide)
    kept = jnp.where(first, wide, zero) if head == 0 else jnp.where(first, zero, wide)
    return kept.astype(LOW)


def parts_of(block):
    return block[:, :128], block[:, 128:256], block[:, 256:]


def same_image(ids):
    row = ids.astype(WIDE)
    return jnp.broadcast_to(row, (8, row.shape[1])).T[:, :1] == row


def attend_kernel(query_ids, triple, mixed, log_total):
    same = same_image(query_ids[0])
    query, keys, values = parts_of(triple[...])
    turned = values.astype(WIDE).T.astype(LOW)
    size = turned.shape[0] // 2
    parts = []
    for head in range(2):
        raw = dot_last(head_of(keys, head), query)
        raw = jnp.where(same, raw, NEGATIVE)
        top = jnp.max(raw, axis=0, keepdims=True)
        expo = jnp.exp2((raw - top) * (SCALE * LOG2E))
        total = jnp.sum(expo, axis=0, keepdims=True)
        probs = (expo * (1.0 / total)).astype(LOW)
        parts.append(dot(turned[head * size : (head + 1) * size], probs))
        log_total[0, 0, head : head + 1, :] = top * (SCALE * LOG2E) + jnp.log2(total)
    mixed[...] = jnp.concatenate(parts, axis=0).T.astype(LOW).astype(WIDE)


def attend(triple, query_ids, start, count):
    pairs = triple.shape[1] // 384
    return call(
        attend_kernel,
        (count, pairs),
        [
            pl.BlockSpec((1, 1, LEN), lambda s, p: (start + s, 0, 0)),
            pl.BlockSpec((LEN, 384), lambda s, p: (start + s, p)),
        ],
        [
            pl.BlockSpec((LEN, 128), lambda s, p: (s, p)),
            pl.BlockSpec((1, 1, 2, LEN), lambda s, p: (s, p, 0, 0)),
        ],
        [
            jax.ShapeDtypeStruct((count * LEN, pairs * 128), WIDE),
            jax.ShapeDtypeStruct((count, pairs, 2, LEN), WIDE),
        ],
        (query_ids, triple),
        flops=count * pairs * LEN * LEN * 1024,
    )


def attend_back_kernel(
    query_ids,
    triple_own,
    triple_rest,
    grad_mixed,
    log_own,
    log_rest,
    weight,
    own_pair,
    own_last,
    partial,
    sums,
):
    pair = pl.program_id(0)
    lead = pair == 0
    same = same_image(query_ids[0])
    block = jnp.where(
        lead, triple_own[...].astype(WIDE), triple_rest[...].astype(WIDE)
    ).astype(LOW)
    log_total = jnp.where(lead, log_own[0, 0], log_rest[0, 0])
    query, keys, values = parts_of(block)
    turned = keys.astype(WIDE).T.astype(LOW)
    size = turned.shape[0] // 2
    grad_query = []
    grad_keys = []
    grad_values = []
    for head in range(2):
        raw = dot_last(head_of(keys, head), query)
        scaled = jnp.where(same, raw * (SCALE * LOG2E), NEGATIVE)
        probs = jnp.exp2(scaled - log_total[head : head + 1, :])
        grad_probs = dot_last(head_of(values, head), grad_mixed[...])
        inner = jnp.sum(probs * grad_probs, axis=0, keepdims=True)
        grad_scores = (probs * (grad_probs - inner)).astype(LOW)
        grad_query.append(dot(turned[head * size : (head + 1) * size], grad_scores))
        grad_keys.append(dot(grad_scores, query))
        grad_values.append(dot(probs.astype(LOW), grad_mixed[...]))
    first = low_head(query)
    grads = jnp.concatenate(
        [
            SCALE * jnp.concatenate(grad_query, axis=0).T,
            SCALE * jnp.where(first, grad_keys[0], grad_keys[1]),
            jnp.where(first, grad_values[0], grad_values[1]),
        ],
        axis=1,
    ).astype(LOW)
    through = dot(grads, weight[...])
    tally(0, sums.at[0], [row_sum(grads.astype(WIDE))])

    @pl.when(lead)
    def _():
        own_pair[...] = grads
        partial[...] = through

    @pl.when(pair == 1)
    def _():
        own_last[...] = jnp.concatenate(
            [part[:, :64].astype(WIDE) for part in parts_of(grads)], axis=1
        ).astype(LOW)

    @pl.when(pair > 0)
    def _():
        partial[...] += through


def attend_back(
    triple_own, triple_rest, query_ids, grad_mixed, log_own, log_rest, weight, seq, shared
):
    rows = triple_own.shape[0]
    model = weight.shape[1]
    pairs = weight.shape[0] // 384

    def rest(p):
        return jnp.maximum(p - 1, 0)

    return call(
        attend_back_kernel,
        (pairs,),
        [
            pl.BlockSpec((1, 1, LEN), lambda p: (seq, 0, 0)),
            pl.BlockSpec((LEN, 384), lambda p: (seq, 0)),
            pl.BlockSpec((LEN, 384), lambda p: (seq, rest(p))),
            pl.BlockSpec((LEN, 128), lambda p: (0, p)),
            pl.BlockSpec((1, 1, 2, LEN), lambda p: (seq, 0, 0, 0)),
            pl.BlockSpec((1, 1, 2, LEN), lambda p: (0, rest(p), 0, 0)),
            pl.BlockSpec((384, model), lambda p: (p, 0)),
        ],
        [
            pl.BlockSpec((LEN, 384), lambda p: (seq, 0)),
            pl.BlockSpec((LEN, 192), lambda p: (seq, 0)),
            pl.BlockSpec((LEN, model), lambda p: (0, 0)),
            pl.BlockSpec((1, 8, 384), lambda p: (p, 0, 0)),
        ],
        [
            jax.ShapeDtypeStruct((rows, 384), LOW),
            jax.ShapeDtypeStruct((rows, 192), LOW),
            jax.ShapeDtypeStruct((LEN, model), WIDE),
            jax.ShapeDtypeStruct((pairs, 8, 384), WIDE),
        ],
        (query_ids, triple_own, triple_rest, grad_mixed, log_own, log_rest, weight),
        flops=pairs * LEN * LEN * 3328,
        shared=((0, shared[0]), (1, shared[1])),
    )


def gelu_parts(values):
    cdf = 0.5 * (1.0 + lax.erf(values * (0.5**0.5)))
    density = jnp.exp(-0.5 * values * values) * ((2.0 * math.pi) ** -0.5)
    return (values * cdf, cdf + values * density)


def middle_kernel(
    tokens,
    mixed_own,
    mixed_rest,
    other_own,
    other_rest,
    proj,
    vectors,
    up,
    up_bias,
    down,
    cotangent,
    middle,
    normed2,
    hidden,
    grad_pre,
    mixed_kept,
    back_give,
    back_keep,
    fed_give,
    fed_keep,
    sums,
):
    mixed = jnp.concatenate(
        [mixed_own[...], mixed_rest[...], other_own[...], other_rest[...]], axis=1
    ).astype(LOW)
    mixed_kept[...] = mixed[:, :192]
    summed = tokens[...].astype(WIDE) + dot(mixed, proj[...]) + vectors[2:3, :]
    middle[...] = summed
    unit, _ = normalize(summed)
    normed = (unit * vectors[3:4, :] + vectors[4:5, :]).astype(LOW)
    normed2[...] = normed
    activated, slope = gelu_parts(dot(normed, up[...]) + up_bias[...])
    kept = activated.astype(LOW)
    hidden[...] = kept
    grad = (dot_last(cotangent[...], down[...]) * slope).astype(LOW)
    grad_pre[...] = grad
    back_keep[...] = dot_last(grad, up[...])
    fed_keep[...] = dot(kept, down[...])

    @pl.when(pl.program_id(0) == 0)
    def _():
        back_give[...] = back_keep[...]
        fed_give[...] = fed_keep[...]

    tally(
        pl.program_id(0),
        sums,
        [row_sum(cotangent[...].astype(WIDE)), row_sum(grad.astype(WIDE))],
    )


def back_norm_kernel(
    chip, far, other_chip, other_far, is_odd, middle, cotangent, vectors, proj, grad_middle, low, grad_mixed, sums
):
    own = pl.program_id(0) == is_odd[0]
    normed_grad = jnp.where(own, chip[...], other_chip[...]) + jnp.where(
        own, far[...], other_far[...]
    )
    unit, inverse = normalize(middle[...])
    piece = cotangent[...].astype(WIDE) + norm_backward(
        normed_grad, unit, inverse, vectors[3:4, :]
    )
    grad_middle[...] = piece
    rounded = piece.astype(LOW)
    low[...] = rounded
    grad_mixed[...] = dot_last(rounded, proj[...]).astype(LOW)
    tally(
        pl.program_id(0),
        sums,
        [row_sum(normed_grad * unit), row_sum(normed_grad), row_sum(piece)],
    )


def final_kernel(partial, other, tokens, grad_middle, vectors, input_grad, sums):
    normed_grad = partial[...] + other[...]
    unit, inverse = normalize(tokens[...].astype(WIDE))
    input_grad[...] = (
        grad_middle[...] + norm_backward(normed_grad, unit, inverse, vectors[0:1, :])
    ).astype(LOW)
    tally(pl.program_id(0), sums, [row_sum(normed_grad * unit), row_sum(normed_grad)])


def output_kernel(chip, far, other_chip, other_far, is_odd, middle, vectors, out):
    own = pl.program_id(0) == is_odd[0]
    fed = jnp.where(own, chip[...], other_chip[...]) + jnp.where(
        own, far[...], other_far[...]
    )
    out[...] = (middle[...] + fed + vectors[5:6, :]).astype(LOW)


def shards(
    count_dp,
    tokens,
    segment_ids,
    first_gain,
    first_shift,
    qkv_weight,
    qv_bias,
    proj_weight,
    proj_bias,
    second_gain,
    second_shift,
    up_weight,
    up_bias,
    down_weight,
    down_bias,
    cotangent,
):
    rows, model = tokens.shape
    local = qv_bias.shape[1] * qv_bias.shape[2]
    hidden_size = up_weight.shape[1]
    count = rows // LEN
    odd = (lax.axis_index("mp") % 2).astype(jnp.int32).reshape(1)

    in_smem = pl.BlockSpec(memory_space=pltpu.SMEM)

    def row(values):
        return values.astype(WIDE).reshape(1, -1)

    def seq_half(width, seq):
        return pl.BlockSpec((HALF, width), lambda i: (2 * seq + i, 0))

    def half(width):
        return pl.BlockSpec((HALF, width), lambda i: (i, 0))

    own_rows = jnp.transpose(qkv_weight, (1, 2, 0))
    own_bias = qv_bias.reshape(2, local).astype(WIDE)
    far_bias = over_x(own_bias)
    dp_odd = (lax.axis_index("dp") % 2).astype(jnp.int32).reshape(1)
    far_first = over_x(jnp.where(dp_odd[0] == 1, own_rows[1], own_rows[0]).astype(WIDE))
    far_third = over_x(own_rows[2].astype(WIDE))
    far_second = over_dp(far_first, count_dp, 0)
    proj_wide = proj_weight.astype(WIDE)
    far_proj = over_x(proj_wide)
    core_proj = over_core(proj_wide)
    core_far_proj = over_core(far_proj)

    vectors = jnp.stack(
        [first_gain, first_shift, proj_bias, second_gain, second_shift, down_bias, down_bias, down_bias]
    ).astype(WIDE)
    vector_spec = whole((8, model))
    query_ids = segment_ids.reshape(count, 1, LEN)
    none = jnp.zeros((128,), WIDE)
    bias_own = row(jnp.concatenate([own_bias[0, :128], none, own_bias[1, :128]]))
    bias_rest = row(
        jnp.concatenate(
            [
                own_bias[0, 128:],
                far_bias[0, :64],
                none,
                own_bias[1, 128:],
                far_bias[1, :64],
                far_bias[0, 64:],
                none,
                far_bias[1, 64:],
            ]
        )
    )

    normed1, triple_own = call(
        front_kernel,
        (2 * count,),
        [
            half(model),
            vector_spec,
            whole((3, 128, model)),
            whole((1, 384)),
        ],
        [half(model), half(384)],
        [jax.ShapeDtypeStruct((rows, model), LOW), jax.ShapeDtypeStruct((rows, 384), LOW)],
        (tokens, vectors, own_rows, bias_own),
        flops=rows * model * 800,
    )
    mixed_own, log_own = attend(triple_own, query_ids, 0, count)
    other_own = over_core(mixed_own)

    triple_rest, weight_six = call(
        rest_kernel,
        (2 * count,),
        [
            half(model),
            whole((3, local, model)),
            whole((local, model)),
            whole((local, model)),
            whole((local, model)),
            in_smem,
            whole((1, 4 * local)),
        ],
        [half(4 * local), whole((3, 3, 128, model))],
        [
            jax.ShapeDtypeStruct((rows, 4 * local), LOW),
            jax.ShapeDtypeStruct((3, 3, 128, model), LOW),
        ],
        (normed1, own_rows, far_first, far_second, far_third, dp_odd, bias_rest),
        flops=rows * model * local * 8,
    )
    weight_six = weight_six.reshape(6 * local, model)
    proj_all = call(
        pack_kernel,
        (1,),
        [whole((local, model))] * 4,
        whole((4 * local, model)),
        jax.ShapeDtypeStruct((4 * local, model), LOW),
        (proj_weight, far_proj, core_proj, core_far_proj),
        flops=4 * local * model,
    )

    def picked(width, seq):
        return pl.BlockSpec(
            (HALF, width), lambda i, is_odd: (2 * seq + (i + 1 + is_odd[0]) % 2, 0)
        )

    attended = []
    for seq in range(count):
        mixed_rest, log_rest = attend(triple_rest, query_ids, seq, 1)
        attended.append((mixed_rest, log_rest, over_core(mixed_rest)))

    kept = [None] * 4
    middles = []
    mlp_sums = []
    back_chip = []
    fed_chip = []
    for seq in range(count):
        mixed_rest, _, other_rest = attended[seq]
        middle, *kept, back_give, back_keep, fed_give, fed_keep, sums = call(
            middle_kernel,
            (2,),
            [
                picked(model, seq),
                picked(128, seq),
                picked(256, 0),
                picked(128, seq),
                picked(256, 0),
                whole((model, model)),
                vector_spec,
                whole((model, hidden_size)),
                whole((1, hidden_size)),
                whole((hidden_size, model)),
                picked(model, seq),
            ],
            [
                picked(model, 0),
                picked(model, seq),
                picked(hidden_size, seq),
                picked(hidden_size, seq),
                picked(local, seq),
                *([whole((HALF, model))] * 4),
                whole((8, model)),
            ],
            [
                jax.ShapeDtypeStruct((LEN, model), WIDE),
                jax.ShapeDtypeStruct((rows, model), LOW),
                jax.ShapeDtypeStruct((rows, hidden_size), LOW),
                jax.ShapeDtypeStruct((rows, hidden_size), LOW),
                jax.ShapeDtypeStruct((rows, local), LOW),
                *([jax.ShapeDtypeStruct((HALF, model), WIDE)] * 4),
                jax.ShapeDtypeStruct((8, model), WIDE),
            ],
            (
                tokens,
                mixed_own,
                mixed_rest,
                other_own,
                other_rest,
                proj_all,
                vectors,
                up_weight,
                row(up_bias),
                down_weight,
                cotangent,
            ),
            flops=LEN * model * model * 10,
            prefetch=odd,
            shared=tuple((1 + i, kept[i]) for i in range(4)),
        )
        middles.append(middle)
        mlp_sums.append(sums)
        back_chip.append(back_keep + over_core(back_give))
        fed_chip.append(fed_keep + over_core(fed_give))
    normed2, hidden, grad_pre, mixed_kept = kept

    back_far = []
    for seq in range(count):
        back_far.append(over_x(back_chip[seq]))
    fed_far = []
    for seq in range(count):
        fed_far.append(over_x(fed_chip[seq]))

    def grad(*operands):
        width = sum(right.shape[1] for right in operands[1::2])
        tile = min(width, TILE)
        block = model // count_dp
        part = pl.BlockSpec((count_dp // 4, block, tile), lambda i, j: (i, 0, j))
        return call(
            functools.partial(grad_kernel, block),
            (2, width // tile),
            [
                pl.BlockSpec((rows, min(values.shape[1], tile)), lambda i, j: (0, j))
                if index % 2
                else pl.BlockSpec((rows, model // 2), lambda i, j: (0, i))
                for index, values in enumerate(operands)
            ]
            + [in_smem],
            [part, part],
            [jax.ShapeDtypeStruct((count_dp // 2, block, width), WIDE)] * 2,
            (*operands, dp_odd),
            flops=2 * rows * model * width,
        )

    down_part = scatter_dp(*grad(cotangent, hidden), count_dp)
    up_part = scatter_dp(*grad(normed2, grad_pre), count_dp)

    low_rows = None
    own_grads = [None, None]
    input_grad = None
    norm_sums = []
    attend_sums = []
    first_sums = []
    for seq in range(count):
        other_chip = over_core(back_chip[seq])
        other_far = over_core(back_far[seq])
        grad_middle, low_rows, grad_mixed, sums = call(
            back_norm_kernel,
            (2,),
            [
                *([whole((HALF, model))] * 4),
                in_smem,
                half(model),
                seq_half(model, seq),
                vector_spec,
                whole((2 * local, model)),
            ],
            [half(model), seq_half(model, seq), half(2 * local), whole((8, model))],
            [
                jax.ShapeDtypeStruct((LEN, model), WIDE),
                jax.ShapeDtypeStruct((rows, model), LOW),
                jax.ShapeDtypeStruct((LEN, 2 * local), LOW),
                jax.ShapeDtypeStruct((8, model), WIDE),
            ],
            (
                back_chip[seq],
                back_far[seq],
                other_chip,
                other_far,
                odd,
                middles[seq],
                cotangent,
                vectors,
                proj_all,
            ),
            flops=LEN * model * local * 8,
            shared=((1, low_rows),),
        )
        norm_sums.append(sums)
        *own_grads, partial, sums = attend_back(
            triple_own,
            triple_rest,
            query_ids,
            grad_mixed,
            log_own,
            attended[seq][1],
            weight_six,
            seq,
            own_grads,
        )
        attend_sums.append(sums)
        other = over_core(partial)

        def part(width):
            return pl.BlockSpec((HALF // 2, width), lambda i: (i, 0))

        def seq_part(width, seq=seq):
            return pl.BlockSpec((HALF // 2, width), lambda i: (4 * seq + i, 0))

        input_grad, sums = call(
            final_kernel,
            (4,),
            [
                part(model),
                part(model),
                seq_part(model),
                part(model),
                vector_spec,
            ],
            [seq_part(model), whole((8, model))],
            [
                jax.ShapeDtypeStruct((rows, model), LOW),
                jax.ShapeDtypeStruct((8, model), WIDE),
            ],
            (partial, other, tokens, grad_middle, vectors),
            flops=LEN * model * 40,
            shared=((0, input_grad),),
        )
        first_sums.append(sums)

    pair_part = scatter_dp(*grad(normed1, own_grads[0]), count_dp)
    last_part = scatter_dp(*grad(normed1, own_grads[1], low_rows, mixed_kept), count_dp)
    proj_part = last_part[:, local:]
    last_part = last_part[:, :local]
    block = pair_part.shape[0]
    qkv_part = jnp.concatenate(
        [pair_part.reshape(block, 3, 128), last_part.reshape(block, 3, 64)], axis=2
    )

    layer_output = None
    for seq in range(count):
        other_chip = over_core(fed_chip[seq])
        other_far = over_core(fed_far[seq])
        layer_output = call(
            output_kernel,
            (2,),
            [
                *([whole((HALF, model))] * 4),
                in_smem,
                half(model),
                vector_spec,
            ],
            seq_half(model, seq),
            jax.ShapeDtypeStruct((rows, model), LOW),
            (fed_chip[seq], fed_far[seq], other_chip, other_far, odd, middles[seq], vectors),
            flops=LEN * model * 4,
            shared=((0, layer_output),),
        )

    mlp_sums = sum(mlp_sums)
    norm_sums = sum(norm_sums)
    attend_sums = sum(attend_sums)[:2, 0]
    first_sums = sum(first_sums)
    pair_sums = attend_sums[0].reshape(3, 128)
    last_sums = attend_sums[1].reshape(3, 128)[:, :64]
    qv_sums = jnp.concatenate([pair_sums, last_sums], axis=1)
    flat = jnp.concatenate(
        [
            first_sums[0],
            first_sums[1],
            norm_sums[2],
            norm_sums[0],
            norm_sums[1],
            mlp_sums[0],
            mlp_sums[1],
            qv_sums[0],
            qv_sums[2],
        ]
    )
    sums = sum_dp(flat, count_dp)
    here = lax.axis_index("dp")

    def share(values, axis):
        size = values.shape[axis] // count_dp
        return lax.dynamic_slice_in_dim(values, here * size, size, axis)

    vectors = share(sums[: 6 * model].reshape(6, model), 1)
    up_bias_sum = sums[6 * model : 6 * model + hidden_size].reshape(up_bias.shape)
    qv_sum = sums[6 * model + hidden_size :].reshape(qv_bias.shape)
    return (
        layer_output,
        input_grad,
        vectors[0],
        vectors[1],
        qkv_part,
        share(qv_sum, 2),
        proj_part.T,
        vectors[2],
        vectors[3],
        vectors[4],
        up_part,
        share(up_bias_sum, 1),
        down_part.T,
        vectors[5],
    )


def solution(mesh):
    count_dp = mesh.shape["dp"]

    def layer(*args):
        return shards(count_dp, *args)

    in_specs = (
        P("dp", None),
        P("dp"),
        P(),
        P(),
        P(None, None, "mp"),
        P(None, "mp", None),
        P("mp", None),
        P(),
        P(),
        P(),
        P(None, "mp"),
        P("mp", None),
        P("mp", None),
        P(),
        P("dp", None),
    )
    out_specs = (
        P("dp", None),
        P("dp", None),
        P("dp"),
        P("dp"),
        P("dp", None, "mp"),
        P(None, "mp", "dp"),
        P("mp", "dp"),
        P("dp"),
        P("dp"),
        P("dp"),
        P("dp", "mp"),
        P("mp", "dp"),
        P("mp", "dp"),
        P("dp"),
    )
    return jax.shard_map(layer, mesh=mesh, in_specs=in_specs, out_specs=out_specs, check_vma=False)
```
